256 devices in a mesh: gx: 16 (over z, x_hi), gy: 8 (over y, core), col: 2 (over x_lo).
Axes of the slice: x: 4 (x_hi: 2, x_lo: 2; x = x_hi * 2 + x_lo), y: 4, z: 8, core: 2. Of those that a mesh axis runs over, the one named last changes fastest.
Arguments:
- sources: float32 [16, 8, 2, 128, 1152], P('gx', 'gy', None, 'col'), may hold values from -100 to 100
- impedance: bfloat16 [16, 8, 2, 1152, 1152], P('gx', 'gy'), may hold values from -0.09375 to 0.09375
- pair_maps: bfloat16 [16, 8, 2, 2, 384, 384], P('gx', 'gy'), may hold values from -0.21875 to 0.21875
- lead_side: int32 [16, 8, 2], P('gx', 'gy'), may hold values from 0 to 1
- coarse_basis: float32 [16, 8, 32, 2, 1152], P('gx', 'gy'), may hold values from -0.125 to 0.125
- coarse_inverse: float32 [4096, 4096], P(('gx', 'gy', 'col')), may hold values from -0.6 to 0.6
Outputs:
- solution_traces: float32 [16, 8, 2, 128, 1152], P('gx', 'gy', None, 'col')
The draws below stay inside these ranges and needn't reach their ends.
Inputs may be any that keep to these rules, and one draw needn't show every extreme that they name: `lead_side`: entries of interfaces beyond the last subdomain along a dimension are read by no step.
All inputs are finite; a program needn't handle non-finite values.
Results may differ from the reference program's by a relative error of at most 0.0039.
Values may be sent and summed in bfloat16 or wider, within the bound.
A program may use at most 64 MiB of HBM per device.

```python
import math
import jax
import jax.numpy as jnp
from jax import lax

FACE = 192
CPS = 32
ITERS = 2
TRACE = 1152
PAIR = 384
SUB_X = 16
SUB_Y = 8
SRC = 128
COARSE = 4096


def draw_sources(key, part):
    subkeys = jax.random.split(jax.random.fold_in(key, 17), 3)
    array_shape = (SUB_X, SUB_Y, 2, SRC, TRACE)
    first_pos = jnp.arange(SUB_X, dtype=jnp.float32) / max(SUB_X - 1, 1)
    second_pos = jnp.arange(SUB_Y, dtype=jnp.float32) / max(SUB_Y - 1, 1)
    growth = 3.0
    entries = jax.random.truncated_normal(subkeys[0], -4.0, 4.0, array_shape, jnp.float32)
    ramp_values = growth ** (first_pos[:, None] + second_pos[None, :] - 1.0)
    col_scale = jnp.exp(jax.random.uniform(subkeys[2], (SUB_X, SUB_Y, 1, 1, TRACE), jnp.float32, math.log(0.5), math.log(2.0)))
    return entries * ramp_values[:, :, None, None, None] * col_scale


def touch_ends(result, rng, low, top_value):
    shape = result.shape
    index_at = [jax.random.randint(jax.random.fold_in(rng, axis), (), 0, shape[axis]) for axis in range(len(shape))]
    result = result.at[tuple(index_at)].set(low)
    longest = shape.index(max(shape))
    index_at[longest] = (index_at[longest] + 1) % shape[longest]
    return result.at[tuple(index_at)].set(top_value)


def steps_of(own_key, extent, shards, smallest, high):
    loudness = 1.0
    for dim, blocks in shards:
        draws = jax.random.uniform(jax.random.fold_in(jax.random.fold_in(own_key, 6), dim), (blocks,), jnp.float32, smallest / len(shards), high / len(shards))
        loudness = loudness * jnp.repeat(jnp.exp(draws), extent[dim] // blocks).reshape((-1,) + (1,) * (len(extent) - 1 - dim))
    return loudness


def centred(rng, extent, deviation, most, cuts=(), kind=jnp.bfloat16):
    array = jax.random.normal(rng, extent, jnp.float32) * deviation
    if len(cuts) > 0:
        array = steps_of(rng, extent, cuts, -0.22, 0.18) * array
    return jnp.clip(array, min=-most, max=most).astype(kind)


def setup_inputs(seed: int = 0) -> dict:
    splits = jax.random.split(jax.random.key(seed), 7)
    return {
        "sources": draw_sources(jax.random.fold_in(splits[6], 71), 0),
        "impedance": centred(splits[1], (SUB_X, SUB_Y, 2, TRACE, TRACE), (4 * TRACE) ** -0.5, 0.09375, ((0, 16), (1, 8))),
        "pair_maps": centred(splits[2], (SUB_X, SUB_Y, 2, 2, PAIR, PAIR), (4 * FACE) ** -0.5, 0.21875, ((0, 16), (1, 8))),
        "lead_side": touch_ends(jax.random.randint(splits[3], (SUB_X, SUB_Y, 2), 0, 2), jax.random.fold_in(splits[3], 1), 0, 1).astype(jnp.int32),
        "coarse_basis": centred(splits[4], (SUB_X, SUB_Y, CPS, 2, TRACE), (2 * TRACE) ** -0.5, 0.125, ((0, 16), (1, 8)), jnp.float32),
        "coarse_inverse": centred(splits[5], (COARSE, COARSE), 0.1, 0.6, ((0, 256),), jnp.float32),
    }


STEP_RATIO = 0.4

def complex_apply(traces, real_part, imag_part):
    first_part = jnp.einsum('...csn,...nm->...csm', traces, real_part, precision=lax.Precision.HIGHEST)
    second_part = jnp.einsum('...csn,...nm->...csm', traces, imag_part, precision=lax.Precision.HIGHEST)
    return jnp.stack([first_part[..., 0, :, :] - second_part[..., 1, :, :], second_part[..., 0, :, :] + first_part[..., 1, :, :]], axis=-3)

def subdomain_map(inputs):
    rounded, map_pair, drive_traces = inputs
    total_sum = complex_apply(rounded.astype(jnp.float32), map_pair[0].astype(jnp.float32), map_pair[1].astype(jnp.float32)) + drive_traces
    return total_sum.astype(jnp.bfloat16)

def interface_solve(lower_side, upper_side, map_pair, leading):
    leading_flags = leading[:, :, None, None, None]
    ordered = jnp.where(leading_flags == 0, jnp.concatenate([lower_side, upper_side], axis=-1), jnp.concatenate([upper_side, lower_side], axis=-1))
    solved = complex_apply(ordered.astype(jnp.float32), map_pair[:, :, 0].astype(jnp.float32), map_pair[:, :, 1].astype(jnp.float32))
    head_part = solved[..., :FACE]
    tail_part = solved[..., FACE:]
    return (jnp.where(leading_flags == 0, head_part, tail_part), jnp.where(leading_flags == 0, tail_part, head_part))

def reference(sources, impedance, pair_maps, lead_side, coarse_basis, coarse_inverse):
    subdomains = SUB_X * SUB_Y
    iterate = jnp.zeros(sources.shape, jnp.float32)
    flat_maps = impedance.reshape((subdomains,) + impedance.shape[2:])
    flat_drive = sources.reshape((subdomains,) + sources.shape[2:])
    unpadded = (0, 0)
    for repeat in range(ITERS):
        rounded = iterate.astype(jnp.bfloat16).reshape(flat_drive.shape)
        outgoing = lax.map(subdomain_map, (rounded, flat_maps, flat_drive)).reshape(sources.shape)
        first_low, first_high = interface_solve(outgoing[:-1, :, :, :, FACE:2 * FACE], outgoing[1:, :, :, :, :FACE], pair_maps[:-1, :, 0], lead_side[:-1, :, 0])
        second_low, second_high = interface_solve(outgoing[:, :-1, :, :, 3 * FACE:4 * FACE], outgoing[:, 1:, :, :, 2 * FACE:3 * FACE], pair_maps[:, :-1, 1], lead_side[:, :-1, 1])
        face_zero = jnp.pad(first_high, ((1, 0), unpadded, unpadded, unpadded, unpadded))
        face_one = jnp.pad(first_low, ((0, 1), unpadded, unpadded, unpadded, unpadded))
        face_two = jnp.pad(second_high, (unpadded, (1, 0), unpadded, unpadded, unpadded))
        face_three = jnp.pad(second_low, (unpadded, (0, 1), unpadded, unpadded, unpadded))
        updated = jnp.concatenate([face_zero, face_one, face_two, face_three, outgoing[..., 5 * FACE:6 * FACE].astype(jnp.float32), outgoing[..., 4 * FACE:5 * FACE].astype(jnp.float32)], axis=-1)
        defect = updated - iterate
        projected = jnp.einsum('abcsk,abpck->absp', defect, coarse_basis, precision=lax.Precision.HIGHEST)
        gathered = projected.reshape(subdomains, SRC, CPS).transpose(1, 0, 2).reshape(SRC, COARSE)
        coarse = jnp.dot(gathered, coarse_inverse.T, precision=lax.Precision.HIGHEST).reshape(SRC, SUB_X, SUB_Y, CPS)
        correction = jnp.einsum('sabp,abpck->abcsk', coarse, coarse_basis, precision=lax.Precision.HIGHEST)
        defect_norm = lax.optimization_barrier(jnp.sum(defect * defect, axis=(0, 1, 2, 4)))
        correction_norm = lax.optimization_barrier(jnp.sum(correction * correction, axis=(0, 1, 2, 4)))
        factor = STEP_RATIO * jnp.sqrt(defect_norm / (correction_norm + 1e-06))
        iterate = updated + factor[None, None, None, :, None] * correction
    return iterate
```

```python
import functools

import jax
import jax.numpy as jnp
from jax import lax
from jax.experimental import pallas as pl
from jax.experimental.pallas import tpu as pltpu
from jax.sharding import PartitionSpec as P

ITERS = 2
STEP_RATIO = 0.4
MESH = pl.DeviceIdType.MESH
F32 = jnp.float32
BF16 = jnp.bfloat16
HIGHEST = lax.Precision.HIGHEST


def dot(a, b, precision=None):
    return jnp.dot(a, b, preferred_element_type=F32, precision=precision)


def dot_nt(a, b, precision=None):
    return lax.dot_general(
        a, b, (((1,), (1,)), ((), ())), preferred_element_type=F32, precision=precision
    )


def dot_tn(a, b):
    return lax.dot_general(a, b, (((0,), (0,)), ((), ())), preferred_element_type=F32)


def split(x):
    high = x.astype(BF16)
    return high, (x - high.astype(F32)).astype(BF16)


def kernel(
    shape,
    lead_ref,
    src_hbm,
    imp_hbm,
    maps_hbm,
    basis_hbm,
    inv_hbm,
    out_ref,
    src,
    imp,
    maps,
    basis,
    inv,
    solver,
    inv_all,
    outgoing,
    face_in,
    ret_out,
    ret_in,
    updated,
    state,
    rows,
    rows_turned,
    product,
    proj_rows,
    basis_k,
    mapped_k,
    gathered,
    sum_z,
    sum_m,
    sum_c,
    load_sem,
    send_sem,
    recv_sem,
):
    nz, nh, ny, nc, ncol = shape
    nm = nh * ny
    ngx, ngy = nz * nh, ny * nc
    sources = src.shape[0] // 2
    trace = src.shape[1]
    face = trace // 6
    pair = 2 * face
    cps = basis.shape[0]
    half = cps // 2

    gx, gy, col = lax.axis_index("gx"), lax.axis_index("gy"), lax.axis_index("col")
    z, xh = gx // nh, gx % nh
    y, core = gy // nc, gy % nc
    m = xh * ny + y

    def at(z_to, m_to, core_to):
        return {
            "gx": z_to * nh + m_to // ny,
            "gy": (m_to % ny) * nc + core_to,
            "col": col,
        }

    z_peers = [at((z + o) % nz, m, core) for o in range(1, nz)]
    m_peers = [at(z, (m + o) % nm, core) for o in range(1, nm)]
    c_peers = [at(z, m, (core + o) % nc) for o in range(1, nc)]
    below = [
        {"gx": (gx + ngx - 1) % ngx, "gy": gy, "col": col},
        {"gx": gx, "gy": (gy + ngy - 1) % ngy, "col": col},
    ]
    above = [
        {"gx": (gx + 1) % ngx, "gy": gy, "col": col},
        {"gx": gx, "gy": (gy + 1) % ngy, "col": col},
    ]
    col_peer = {"gx": gx, "gy": gy, "col": (col + 1) % ncol}
    position, last = [gx, gy], [ngx - 1, ngy - 1]

    loads = [
        pltpu.make_async_copy(a, b, load_sem.at[i])
        for i, (a, b) in enumerate(
            [(src_hbm, src), (maps_hbm, maps), (basis_hbm, basis), (inv_hbm, inv), (imp_hbm, imp)]
        )
    ]
    for load in loads:
        load.start()

    barrier = pltpu.get_barrier_semaphore()
    partners = z_peers + m_peers + c_peers + below + above + [col_peer]
    for partner in partners:
        pl.semaphore_signal(barrier, inc=1, device_id=partner, device_id_type=MESH)

    sent = []

    def remote(source, target, device):
        k = len(sent)
        copy = pltpu.make_async_remote_copy(
            src_ref=source,
            dst_ref=target,
            send_sem=send_sem.at[k],
            recv_sem=recv_sem.at[k],
            device_id=device,
            device_id_type=MESH,
        )
        copy.start()
        sent.append(copy)
        return copy

    def arrive(copies):
        for copy in copies:
            copy.wait_recv()

    lane = lax.broadcasted_iota(jnp.int32, (2 * sources, 128), 1)
    small_lane = lax.broadcasted_iota(jnp.int32, (half, 128), 1)

    loads[0].wait()
    outgoing[...] = src[...].astype(BF16)
    pl.semaphore_wait(barrier, len(partners))

    def send_faces(it):
        return [
            remote(outgoing.at[:, pl.ds(d * pair, 256)], face_in.at[it, d], below[d])
            for d in range(2)
        ]

    def turned(x):
        return jnp.concatenate([-x[sources:], x[:sources]], axis=0)

    def exchange(it, coming):
        returned, own = [], []
        for d in range(2):
            coming[d].wait_recv()
            upper = face_in[it, d]
            here = outgoing[:, pl.ds(d * pair, pair)]
            middle = jnp.where(
                lane < 64, upper[:, 128:].astype(F32), here[:, 128:256].astype(F32)
            ).astype(BF16)
            x = jnp.concatenate([upper[:, :128], middle, here[:, 256:]], axis=1)
            solved = dot(x, solver[d, 0]) + dot(turned(x), solver[d, 1])
            ret_out[it, d] = solved[:, :256].astype(BF16)
            returned.append(remote(ret_out.at[it, d], ret_in.at[it, d], above[d]))
            own.append(jnp.where(position[d] < last[d], solved[:, 128:], 0.0))
        ends = outgoing[:, pl.ds(2 * pair, pair)].astype(F32)
        updated[:, pl.ds(2 * pair, pair)] = pltpu.roll(ends, face, 1)
        for d in range(2):
            returned[d].wait_recv()
            back = jnp.where(position[d] > 0, ret_in[it, d].astype(F32), 0.0)
            updated[:, pl.ds(d * pair, 128)] = back[:, :128]
            updated[:, pl.ds(d * pair + 128, 128)] = jnp.where(
                lane < 64, back[:, 128:], own[d][:, :128]
            )
            updated[:, pl.ds(d * pair + 256, 128)] = own[d][:, 128:]

    def project(defect):
        high, low = split(defect)
        first = dot_nt(proj_rows[...], high)
        second = dot_nt(proj_rows[pl.ds(0, 2 * cps), :], low)
        by_part = first[: 2 * cps] + first[2 * cps :] + second
        total = by_part[:cps] + pltpu.roll(by_part[cps:], sources, 1)
        return jnp.where(
            small_lane < 64, total[:half], pltpu.roll(total[half:], sources, 1)
        ).astype(BF16)

    def squares(defect):
        sq = defect * defect
        folded = sq[:, :128]
        for t in range(1, trace // 128):
            folded = folded + sq[:, 128 * t : 128 * (t + 1)]
        folded = folded[:sources] + folded[sources:]
        both = jnp.concatenate([folded, folded], axis=0)
        return dot_nt(jnp.ones((8, 128), F32), both, HIGHEST)

    def gather_z(it, packed):
        gathered[it, z, m, core] = packed
        block = gathered.at[it, z, m, core]
        return [remote(block, block, peer) for peer in z_peers]

    def gather_m(it, coming):
        arrive(coming)
        block = gathered.at[it, :, m, core]
        return [remote(block, block, peer) for peer in m_peers]

    def gather_c(it, coming):
        arrive(coming)
        block = gathered.at[it, :, :, core]
        arrive([remote(block, block, peer) for peer in c_peers])

    def coarse_of(it):
        whole = gathered[it].reshape(-1, 128)
        parts = dot(inv_all[...].reshape(2 * cps, whole.shape[0]), whole)
        return parts[:cps] + pltpu.roll(parts[cps:], sources, 1)

    def total_of(it, row):
        for buffer, index, peers in ((sum_z, z, z_peers), (sum_m, m, m_peers), (sum_c, core, c_peers)):
            buffer[it, index] = row
            arrive([remote(buffer.at[it, index], buffer.at[it, index], peer) for peer in peers])
            row = buffer[it, 0]
            for i in range(1, buffer.shape[1]):
                row = row + buffer[it, i]
        return row

    def stacked(coefficients):
        high, low = split(coefficients)
        return jnp.concatenate([high, low, high], axis=0)[:, :sources]

    def factor_of(total):
        factor = STEP_RATIO * jnp.sqrt(total / (pltpu.roll(total, sources, 1) + 1e-06))
        return factor[0:1]

    def stack_k(target, block):
        for c in range(2):
            high, low = split(block[c * cps : (c + 1) * cps])
            target[c, pl.ds(0, cps)] = high
            target[c, pl.ds(cps, cps)] = high
            target[c, pl.ds(2 * cps, cps)] = low

    faces = send_faces(0)

    loads[1].wait()
    for d in range(2):
        for c in range(2):
            stored = maps[2 * d + c].astype(F32)
            swapped = jnp.concatenate([stored[face:], stored[:face]], axis=0)
            swapped = pltpu.roll(swapped, face, 1)
            solver[d, c] = jnp.where(lead_ref[d] == 0, swapped, stored).astype(BF16)

    loads[2].wait()
    both = jnp.concatenate([basis[:, 0, :], basis[:, 1, :]], axis=0)
    high, low = split(both)
    proj_rows[pl.ds(0, 2 * cps), :] = high
    proj_rows[pl.ds(2 * cps, 2 * cps), :] = low
    stack_k(basis_k, both)
    base = 2 * sources
    for part, block in enumerate((high, low)):
        rows[pl.ds(base + part * 2 * cps, 2 * cps), :] = block
        rows_turned[pl.ds(base + part * 2 * cps, 2 * cps), :] = jnp.concatenate(
            [-block[cps:], block[:cps]], axis=0
        )
    gram = dot_nt(both[:cps], both[:cps], HIGHEST) + dot_nt(both[cps:], both[cps:], HIGHEST)

    loads[3].wait()
    here = lax.broadcasted_iota(jnp.int32, (256, 256), 0)
    there = lax.broadcasted_iota(jnp.int32, (256, 256), 1)
    wanted = ((here // half) % 2) * 128 + (here // cps) * half + here % half
    order = jnp.where(there == wanted, 1.0, 0.0).astype(BF16)
    for j in range(inv.shape[1] // 256):
        moved = dot(inv[:, 256 * j : 256 * (j + 1)].astype(BF16), order).astype(BF16)
        for h in range(2):
            inv_all[h, col, :, pl.ds(128 * j, 128)] = moved[:, 128 * h : 128 * (h + 1)]
    inverse_coming = remote(inv_all.at[:, col], inv_all.at[:, col], col_peer)

    exchange(0, faces)

    first_updated = updated[...]
    coming = gather_z(0, project(first_updated))
    first_squares = squares(first_updated)
    high = first_updated.astype(BF16)
    rows[pl.ds(0, base), :] = high
    rows_turned[pl.ds(0, base), :] = turned(high)
    loads[4].wait()
    for j in range(trace // 384):
        span = pl.ds(384 * j, 384)
        product[:, span] = dot(rows[...], imp[pl.ds(0, trace), span]) + dot(
            rows_turned[...], imp[pl.ds(trace, trace), span]
        )
    coming = gather_m(0, coming)
    mapped = product[pl.ds(base, 2 * cps), :] + product[pl.ds(base + 2 * cps, 2 * cps), :]
    stack_k(mapped_k, mapped)
    gather_c(0, coming)
    inverse_coming.wait_recv()

    def scaled_coarse(it, norm):
        coarse = coarse_of(it)
        energy = jnp.sum(coarse * dot(gram, coarse, HIGHEST), axis=0, keepdims=True)
        wide_lane = lax.broadcasted_iota(jnp.int32, (8, 128), 1)
        row = jnp.where(
            wide_lane < 64, norm, pltpu.roll(jnp.broadcast_to(energy, (8, 128)), sources, 1)
        )
        return stacked(coarse * factor_of(total_of(it, row)))

    scaled = scaled_coarse(0, first_squares)
    for copy in faces:
        copy.wait_send()
    for c in range(2):
        part = pl.ds(c * sources, sources)
        outgoing[part, :] = (
            product[part, :] + src[part, :] + dot_tn(scaled, mapped_k[c])
        ).astype(BF16)
    coming = send_faces(1)
    for c in range(2):
        part = pl.ds(c * sources, sources)
        state[part, :] = updated[part, :] + dot_tn(scaled, basis_k[c])
    exchange(1, coming)
    defect = updated[...] - state[...]
    coming = gather_z(1, project(defect))
    second_squares = squares(defect)
    coming = gather_m(1, coming)
    gather_c(1, coming)
    scaled = scaled_coarse(1, second_squares)
    for c in range(2):
        part = pl.ds(c * sources, sources)
        out_ref[part, :] = updated[part, :] + dot_tn(scaled, basis_k[c])
    for copy in sent[len(faces) :]:
        copy.wait_send()


def per_device(shape, sources, impedance, pair_maps, lead_side, coarse_basis, coarse_inverse):
    nz, nh, ny, nc, ncol = shape
    here, trace = sources.shape[3], sources.shape[4]
    pair = pair_maps.shape[-1]
    cps = coarse_basis.shape[2]
    size = coarse_inverse.shape[1]
    nm = nh * ny
    copies = 1 + ITERS * (4 + 2 * (nz - 1 + nm - 1 + nc - 1))
    hbm = pl.BlockSpec(memory_space=pl.ANY)
    out = pl.pallas_call(
        functools.partial(kernel, shape),
        out_shape=jax.ShapeDtypeStruct((2 * here, trace), F32),
        in_specs=[pl.BlockSpec(memory_space=pltpu.SMEM)] + [hbm] * 5,
        out_specs=pl.BlockSpec(memory_space=pltpu.VMEM),
        scratch_shapes=[
            pltpu.VMEM((2 * here, trace), F32),
            pltpu.VMEM((2 * trace, trace), BF16),
            pltpu.VMEM((4, pair, pair), BF16),
            pltpu.VMEM((cps, 2, trace), F32),
            pltpu.VMEM((cps // 2, size), F32),
            pltpu.VMEM((2, 2, pair, pair), BF16),
            pltpu.VMEM((2, ncol, cps // 2, size // 2), BF16),
            pltpu.VMEM((2 * here, trace), BF16),
            pltpu.VMEM((ITERS, 2, 2 * here, 256), BF16),
            pltpu.VMEM((ITERS, 2, 2 * here, 256), BF16),
            pltpu.VMEM((ITERS, 2, 2 * here, 256), BF16),
            pltpu.VMEM((2 * here, trace), F32),
            pltpu.VMEM((2 * here, trace), F32),
            pltpu.VMEM((2 * here + 4 * cps, trace), BF16),
            pltpu.VMEM((2 * here + 4 * cps, trace), BF16),
            pltpu.VMEM((2 * here + 4 * cps, trace), F32),
            pltpu.VMEM((4 * cps, trace), BF16),
            pltpu.VMEM((2, 3 * cps, trace), BF16),
            pltpu.VMEM((2, 3 * cps, trace), BF16),
            pltpu.VMEM((ITERS, nz, nm, nc, cps // 2, 128), BF16),
            pltpu.VMEM((ITERS, nz, 8, 128), F32),
            pltpu.VMEM((ITERS, nm, 8, 128), F32),
            pltpu.VMEM((ITERS, nc, 8, 128), F32),
            pltpu.SemaphoreType.DMA((5,)),
            pltpu.SemaphoreType.DMA((copies,)),
            pltpu.SemaphoreType.DMA((copies,)),
        ],
        compiler_params=pltpu.CompilerParams(
            collective_id=0, has_side_effects=True, vmem_limit_bytes=60 * 1024 * 1024
        ),
    )(
        lead_side.reshape(2),
        sources.reshape(2 * here, trace),
        impedance.reshape(2 * trace, trace),
        pair_maps.reshape(4, pair, pair),
        coarse_basis[0, 0],
        coarse_inverse,
    )
    return out.reshape(1, 1, 2, here, trace)


SHAPE = (8, 2, 4, 2, 2)


def build(mesh, shape):
    return jax.shard_map(
        functools.partial(per_device, shape),
        mesh=mesh,
        in_specs=(
            P("gx", "gy", None, "col", None),
            P("gx", "gy", None, None, None),
            P("gx", "gy", None, None, None, None),
            P("gx", "gy", None),
            P("gx", "gy", None, None, None),
            P(("gx", "gy", "col"), None),
        ),
        out_specs=P("gx", "gy", None, "col", None),
        check_vma=False,
    )


def solution(mesh):
    return build(mesh, SHAPE)
```

```python
import functools

import jax
import jax.numpy as jnp
from jax import lax
from jax.experimental import pallas as pl
from jax.experimental.pallas import tpu as pltpu
from jax.sharding import PartitionSpec as P

STEP_RATIO = 0.4
MESH = pl.DeviceIdType.MESH
F32 = jnp.float32
BF16 = jnp.bfloat16
HIGHEST = lax.Precision.HIGHEST


def dot(a, b, precision=None):
    return jnp.dot(a, b, preferred_element_type=F32, precision=precision)


def dot_nt(a, b, precision=None):
    return lax.dot_general(
        a, b, (((1,), (1,)), ((), ())), preferred_element_type=F32, precision=precision
    )


def dot_tn(a, b):
    return lax.dot_general(a, b, (((0,), (0,)), ((), ())), preferred_element_type=F32)


def split(x):
    high = x.astype(BF16)
    return high, (x - high.astype(F32)).astype(BF16)


def kernel(
    shape,
    lead_ref,
    src_hbm,
    imp_hbm,
    maps_hbm,
    basis_hbm,
    inv_hbm,
    out_ref,
    src,
    imp,
    maps,
    basis,
    inv,
    solver,
    inv_all,
    outgoing,
    image_out,
    face_in,
    image_in,
    ret_out,
    ret_in,
    solved_own,
    updated,
    state,
    rows,
    rows_turned,
    product,
    image,
    image_solved,
    proj_rows,
    basis_k,
    mapped,
    mapped_near,
    mapped_k,
    mapped_end,
    kernel_t,
    near_out,
    near_in,
    gathered,
    sum_z,
    sum_m,
    sum_c,
    load_sem,
    send_sem,
    recv_sem,
):
    nz, nh, ny, nc, ncol = shape
    nm = nh * ny
    ngx, ngy = nz * nh, ny * nc
    sources = src.shape[0] // 2
    trace = src.shape[1]
    face = trace // 6
    pair = 2 * face
    cps = basis.shape[0]
    half = cps // 2

    gx, gy, col = lax.axis_index("gx"), lax.axis_index("gy"), lax.axis_index("col")
    z, xh = gx // nh, gx % nh
    y, core = gy // nc, gy % nc
    m = xh * ny + y

    def at(z_to, m_to, core_to):
        return {
            "gx": z_to * nh + m_to // ny,
            "gy": (m_to % ny) * nc + core_to,
            "col": col,
        }

    z_peers = [at((z + o) % nz, m, core) for o in range(1, nz)]
    m_peers = [at(z, (m + o) % nm, core) for o in range(1, nm)]
    c_peers = [at(z, m, (core + o) % nc) for o in range(1, nc)]
    below = [
        {"gx": (gx + ngx - 1) % ngx, "gy": gy, "col": col},
        {"gx": gx, "gy": (gy + ngy - 1) % ngy, "col": col},
    ]
    above = [
        {"gx": (gx + 1) % ngx, "gy": gy, "col": col},
        {"gx": gx, "gy": (gy + 1) % ngy, "col": col},
    ]
    col_peer = {"gx": gx, "gy": gy, "col": (col + 1) % ncol}
    position, last = [gx, gy], [ngx - 1, ngy - 1]

    loads = [
        pltpu.make_async_copy(a, b, load_sem.at[i])
        for i, (a, b) in enumerate(
            [(src_hbm, src), (maps_hbm, maps), (basis_hbm, basis), (inv_hbm, inv), (imp_hbm, imp)]
        )
    ]
    for load in loads:
        load.start()

    barrier = pltpu.get_barrier_semaphore()
    partners = z_peers + m_peers + c_peers + below + above + [col_peer]
    for partner in partners:
        pl.semaphore_signal(barrier, inc=1, device_id=partner, device_id_type=MESH)

    sent = []

    def remote(source, target, device):
        k = len(sent)
        copy = pltpu.make_async_remote_copy(
            src_ref=source,
            dst_ref=target,
            send_sem=send_sem.at[k],
            recv_sem=recv_sem.at[k],
            device_id=device,
            device_id_type=MESH,
        )
        copy.start()
        sent.append(copy)
        return copy

    def arrive(copies):
        for copy in copies:
            copy.wait_recv()

    def lanes(n):
        return lax.broadcasted_iota(jnp.int32, (n, 128), 1)

    def turned(x):
        part = x.shape[0] // 2
        return jnp.concatenate([-x[part:], x[:part]], axis=0)

    def send_faces(it):
        return [
            remote(outgoing.at[it, :, pl.ds(d * pair, 256)], face_in.at[it, d], below[d])
            for d in range(2)
        ]

    def solve(it, d, coming):
        coming[d].wait_recv()
        upper = face_in[it, d]
        here = outgoing[it, :, pl.ds(d * pair, pair)]
        middle = jnp.where(
            lanes(2 * sources) < 64, upper[:, 128:].astype(F32), here[:, 128:256].astype(F32)
        ).astype(BF16)
        x = jnp.concatenate([upper[:, :128], middle, here[:, 256:]], axis=1)
        solved = dot(x, solver[d, 0]) + dot(turned(x), solver[d, 1])
        ret_out[it, d] = solved[:, :256].astype(BF16)
        solved_own[d] = solved[:, 128:]
        return remote(ret_out.at[it, d], ret_in.at[it, d], above[d])

    def assemble(it, returned):
        ends = outgoing[it, :, pl.ds(2 * pair, pair)].astype(F32)
        updated[it, :, pl.ds(2 * pair, pair)] = pltpu.roll(ends, face, 1)
        for d in range(2):
            returned[d].wait_recv()
            back = jnp.where(position[d] > 0, ret_in[it, d].astype(F32), 0.0)
            own = jnp.where(position[d] < last[d], solved_own[d], 0.0)
            updated[it, :, pl.ds(d * pair, 128)] = back[:, :128]
            updated[it, :, pl.ds(d * pair + 128, 128)] = jnp.where(
                lanes(2 * sources) < 64, back[:, 128:], own[:, :128]
            )
            updated[it, :, pl.ds(d * pair + 256, 128)] = own[:, 128:]

    def apply_map(j):
        span = pl.ds(384 * j, 384)
        return dot(rows[...], imp[pl.ds(0, trace), span]) + dot(
            rows_turned[...], imp[pl.ds(trace, trace), span]
        )

    def packed(total):
        return jnp.where(
            lanes(half) < 64, total[:half], pltpu.roll(total[half:], sources, 1)
        ).astype(BF16)

    def project(defect):
        high, low = split(defect)
        first = dot_nt(proj_rows[...], high)
        second = dot_nt(proj_rows[pl.ds(0, 2 * cps), :], low)
        by_part = first[: 2 * cps] + first[2 * cps :] + second
        return packed(by_part[:cps] + pltpu.roll(by_part[cps:], sources, 1))

    def source_sums(products):
        folded = products[:, :128]
        for t in range(1, trace // 128):
            folded = folded + products[:, 128 * t : 128 * (t + 1)]
        folded = folded[:sources] + folded[sources:]
        both = jnp.concatenate([folded, folded], axis=0)
        return dot_nt(jnp.ones((8, 128), F32), both, HIGHEST)

    def gather_z(it, block):
        gathered[it, z, m, core] = block
        own = gathered.at[it, z, m, core]
        return [remote(own, own, peer) for peer in z_peers]

    def gather_m(it, coming):
        arrive(coming)
        block = gathered.at[it, :, m, core]
        return [remote(block, block, peer) for peer in m_peers]

    def gather_c(it, coming):
        arrive(coming)
        block = gathered.at[it, :, :, core]
        return [remote(block, block, peer) for peer in c_peers]

    def coarse_of(it, coming):
        arrive(coming)
        whole = gathered[it].reshape(-1, 128)
        parts = dot(inv_all[...].reshape(2 * cps, whole.shape[0]), whole)
        return parts[:cps] + pltpu.roll(parts[cps:], sources, 1)

    def share(buffer, it, index, peers, row):
        buffer[it, index] = row
        own = buffer.at[it, index]
        return [remote(own, own, peer) for peer in peers]

    def added(buffer, it, coming):
        arrive(coming)
        row = buffer[it, 0]
        for i in range(1, buffer.shape[1]):
            row = row + buffer[it, i]
        return row

    def stacked(coefficients):
        high, low = split(coefficients)
        return jnp.concatenate([high, low, high], axis=0)[:, :sources]

    def factor_of(total):
        return STEP_RATIO * jnp.sqrt(total / (pltpu.roll(total, sources, 1) + 1e-06))

    def energy_of(coarse):
        energy = jnp.sum(coarse * dot(gram, coarse, HIGHEST), axis=0, keepdims=True)
        return pltpu.roll(jnp.broadcast_to(energy, (8, 128)), sources, 1)

    def three(block):
        high, low = split(block)
        return jnp.concatenate([high, high, low], axis=0)

    def mapped_sum(near, c, d):
        if d == 2:
            return dot_tn(stacked(near[0]), mapped_end[c])
        coefficients = jnp.concatenate(
            [stacked(near[0]), stacked(near[1 + 2 * d]), stacked(near[2 + 2 * d])], axis=0
        )
        return dot_tn(coefficients, mapped_k[c, d])

    loads[0].wait()
    outgoing[0] = src[...].astype(BF16)
    pl.semaphore_wait(barrier, len(partners))
    faces = send_faces(0)

    loads[1].wait()
    for d in range(2):
        for c in range(2):
            stored = maps[2 * d + c].astype(F32)
            swapped = jnp.concatenate([stored[face:], stored[:face]], axis=0)
            swapped = pltpu.roll(swapped, face, 1)
            solver[d, c] = jnp.where(lead_ref[d] == 0, swapped, stored).astype(BF16)
    loads[2].wait()
    both = jnp.concatenate([basis[:, 0, :], basis[:, 1, :]], axis=0)
    high, low = split(both)
    proj_rows[pl.ds(0, 2 * cps), :] = high
    proj_rows[pl.ds(2 * cps, 2 * cps), :] = low
    for part, block in enumerate((high, low)):
        rows[pl.ds(part * 2 * cps, 2 * cps), :] = block
        rows_turned[pl.ds(part * 2 * cps, 2 * cps), :] = turned(block)
    returned = [solve(0, d, faces) for d in range(2)]

    loads[4].wait()
    for j in range(trace // 384):
        whole = apply_map(j)
        whole = whole[: 2 * cps] + whole[2 * cps :]
        image[:, pl.ds(384 * j, 384)] = whole
        image_out[:, pl.ds(384 * j, 384)] = whole.astype(BF16)
    assemble(0, returned)

    coming = gather_z(0, project(updated[0]))
    image_coming = [
        remote(image_out.at[:, pl.ds(d * pair, 256)], image_in.at[d], below[d]) for d in range(2)
    ]
    high = updated[0].astype(BF16)
    rows[...] = high
    rows_turned[...] = turned(high)
    for j in range(trace // 384):
        span = pl.ds(384 * j, 384)
        outgoing[1, :, span] = (apply_map(j) + src[:, span]).astype(BF16)
    faces_next = send_faces(1)
    coming = gather_m(0, coming)

    loads[3].wait()
    here = lax.broadcasted_iota(jnp.int32, (256, 256), 0)
    there = lax.broadcasted_iota(jnp.int32, (256, 256), 1)
    wanted = ((here // half) % 2) * 128 + (here // cps) * half + here % half
    order = jnp.where(there == wanted, 1.0, 0.0).astype(BF16)
    for j in range(inv.shape[1] // 256):
        moved = dot(inv[:, 256 * j : 256 * (j + 1)].astype(BF16), order).astype(BF16)
        for h in range(2):
            inv_all[h, col, :, pl.ds(128 * j, 128)] = moved[:, 128 * h : 128 * (h + 1)]
    inverse_coming = remote(inv_all.at[:, col], inv_all.at[:, col], col_peer)

    image_returned = []
    for d in range(2):
        image_coming[d].wait_recv()
        upper = image_in[d].astype(F32)
        own = image_out[:, pl.ds(d * pair, pair)].astype(F32)
        low_lane = lanes(2 * cps) < 64
        zero = jnp.zeros((2 * cps, 128), F32)
        x = jnp.concatenate(
            [zero, jnp.where(low_lane, 0.0, own[:, 128:256]), own[:, 256:]], axis=1
        ).astype(BF16)
        w = jnp.concatenate(
            [upper[:, :128], jnp.where(low_lane, upper[:, 128:], 0.0), zero], axis=1
        ).astype(BF16)
        solved = dot(jnp.concatenate([x, w], axis=0), solver[d, 0]) + dot(
            jnp.concatenate([turned(x), turned(w)], axis=0), solver[d, 1]
        )
        ret_out[2, d] = solved[:, :256].astype(BF16)
        image_solved[d] = solved[:, 128:]
        image_returned.append(remote(ret_out.at[2, d], ret_in.at[2, d], above[d]))
    first_squares = source_sums(updated[0] * updated[0])
    gram = dot_nt(both[:cps], both[:cps], HIGHEST) + dot_nt(both[cps:], both[cps:], HIGHEST)
    for c in range(2):
        basis_k[c] = three(both[c * cps : (c + 1) * cps])
    returned = [solve(1, d, faces_next) for d in range(2)]
    coming = gather_c(0, coming)

    inverse_coming.wait_recv()
    coarse = coarse_of(0, coming)
    high, low = split(coarse)
    near_out[...] = jnp.where(
        lanes(cps) < 64, high.astype(F32), pltpu.roll(low.astype(F32), sources, 1)
    ).astype(BF16)
    near_coming = []
    for d in range(2):
        near_coming.append(remote(near_out, near_in.at[2 * d], above[d]))
        near_coming.append(remote(near_out, near_in.at[2 * d + 1], below[d]))
    first_row = jnp.where(lanes(8) < 64, first_squares, energy_of(coarse))

    assemble(1, returned)
    state[...] = updated[1] - updated[0]
    early = gather_z(2, project(state[...]))
    for d in range(2):
        image_returned[d].wait_recv()
        back = jnp.where(position[d] > 0, ret_in[2, d].astype(F32), 0.0)
        own = jnp.where(position[d] < last[d], image_solved[d], 0.0)
        for target, r, o in ((mapped, 2 * cps, 0), (mapped_near, 0, 2 * cps)):
            target[:, pl.ds(d * pair, 128)] = back[r : r + 2 * cps, :128]
            target[:, pl.ds(d * pair + 128, 128)] = jnp.where(
                lanes(2 * cps) < 64, back[r : r + 2 * cps, 128:], own[o : o + 2 * cps, :128]
            )
            target[:, pl.ds(d * pair + 256, 128)] = own[o : o + 2 * cps, 128:]
    mapped[:, pl.ds(2 * pair, pair)] = pltpu.roll(image[:, pl.ds(2 * pair, pair)], face, 1)
    moved = mapped[...] - both
    blocks = [
        dot_nt(moved[:cps], both[:cps], HIGHEST) + dot_nt(moved[cps:], both[cps:], HIGHEST)
    ]
    left = lax.broadcasted_iota(jnp.int32, (cps, pair), 1) < face
    for d in range(2):
        total = 0.0
        for c in range(2):
            part = mapped_near[pl.ds(c * cps, cps), pl.ds(d * pair, pair)]
            sides = jnp.concatenate([jnp.where(left, part, 0.0), jnp.where(left, 0.0, part)], axis=0)
            total = total + dot_nt(
                sides, both[c * cps : (c + 1) * cps, d * pair : (d + 1) * pair], HIGHEST
            )
            own = three(mapped[pl.ds(c * cps, cps), pl.ds(d * pair, pair)])
            mapped_k[c, d] = jnp.concatenate(
                [own, three(sides[:cps]), three(sides[cps:])], axis=0
            )
        blocks.append(total)
    for c in range(2):
        mapped_end[c] = three(mapped[pl.ds(c * cps, cps), pl.ds(2 * pair, pair)])
    kernel_t[...] = jnp.concatenate(blocks, axis=0).T

    arrive(near_coming)
    near = [coarse]
    for i in range(4):
        both_parts = near_in[i].astype(F32)
        near.append(both_parts + pltpu.roll(both_parts, sources, 1))
    late = gather_z(1, packed(dot(kernel_t[...], jnp.concatenate(near, axis=0), HIGHEST)))
    norms = share(sum_z, 0, z, z_peers, first_row)
    early = gather_m(2, early)
    for c in range(2):
        part = pl.ds(c * sources, sources)
        for d in range(3):
            product[part, pl.ds(d * pair, pair)] = mapped_sum(near, c, d)
        product[part, :] = product[part, :] - dot_tn(stacked(coarse), basis_k[c])
    late = gather_m(1, late)
    norms = share(sum_m, 0, m, m_peers, added(sum_z, 0, norms))
    sums_aa = source_sums(state[...] * state[...])
    sums_ab = source_sums(state[...] * product[...])
    sums_bb = source_sums(product[...] * product[...])
    early = gather_c(2, early)
    coarse_early = coarse_of(2, early)
    late = gather_c(1, late)
    norms = share(sum_c, 0, core, c_peers, added(sum_m, 0, norms))
    factor = factor_of(added(sum_c, 0, norms))
    coarse = coarse_early + factor[0:1] * coarse_of(1, late)
    squares = sums_aa + factor * (2.0 * sums_ab + factor * sums_bb)
    row = jnp.where(lanes(8) < 64, squares, energy_of(coarse))
    norms = share(sum_z, 1, z, z_peers, row)
    near = [factor[0:1] * part for part in near]
    for c in range(2):
        part = pl.ds(c * sources, sources)
        for d in range(3):
            span = pl.ds(d * pair, pair)
            updated[1, part, span] = updated[1, part, span] + mapped_sum(near, c, d)
    norms = share(sum_m, 1, m, m_peers, added(sum_z, 1, norms))
    norms = share(sum_c, 1, core, c_peers, added(sum_m, 1, norms))
    factor = factor_of(added(sum_c, 1, norms))
    scaled = stacked(factor[0:1] * coarse)
    for c in range(2):
        part = pl.ds(c * sources, sources)
        out_ref[part, :] = updated[1, part, :] + dot_tn(scaled, basis_k[c])
    for copy in sent:
        copy.wait_send()


def per_device(shape, sources, impedance, pair_maps, lead_side, coarse_basis, coarse_inverse):
    nz, nh, ny, nc, ncol = shape
    here, trace = sources.shape[3], sources.shape[4]
    pair = pair_maps.shape[-1]
    cps = coarse_basis.shape[2]
    size = coarse_inverse.shape[1]
    nm = nh * ny
    copies = 1 + 3 * 4 + 4 + 5 * (nz - 1 + nm - 1 + nc - 1)
    hbm = pl.BlockSpec(memory_space=pl.ANY)
    out = pl.pallas_call(
        functools.partial(kernel, shape),
        out_shape=jax.ShapeDtypeStruct((2 * here, trace), F32),
        in_specs=[pl.BlockSpec(memory_space=pltpu.SMEM)] + [hbm] * 5,
        out_specs=pl.BlockSpec(memory_space=pltpu.VMEM),
        scratch_shapes=[
            pltpu.VMEM((2 * here, trace), F32),
            pltpu.VMEM((2 * trace, trace), BF16),
            pltpu.VMEM((4, pair, pair), BF16),
            pltpu.VMEM((cps, 2, trace), F32),
            pltpu.VMEM((cps // 2, size), F32),
            pltpu.VMEM((2, 2, pair, pair), BF16),
            pltpu.VMEM((2, ncol, cps // 2, size // 2), BF16),
            pltpu.VMEM((2, 2 * here, trace), BF16),
            pltpu.VMEM((2 * cps, trace), BF16),
            pltpu.VMEM((2, 2, 2 * here, 256), BF16),
            pltpu.VMEM((2, 2 * cps, 256), BF16),
            pltpu.VMEM((3, 2, 2 * here, 256), BF16),
            pltpu.VMEM((3, 2, 2 * here, 256), BF16),
            pltpu.VMEM((2, 2 * here, 256), F32),
            pltpu.VMEM((2, 2 * here, trace), F32),
            pltpu.VMEM((2 * here, trace), F32),
            pltpu.VMEM((2 * here, trace), BF16),
            pltpu.VMEM((2 * here, trace), BF16),
            pltpu.VMEM((2 * here, trace), F32),
            pltpu.VMEM((2 * cps, trace), F32),
            pltpu.VMEM((2, 4 * cps, 256), F32),
            pltpu.VMEM((4 * cps, trace), BF16),
            pltpu.VMEM((2, 3 * cps, trace), BF16),
            pltpu.VMEM((2 * cps, trace), F32),
            pltpu.VMEM((2 * cps, 2 * pair), F32),
            pltpu.VMEM((2, 2, 9 * cps, pair), BF16),
            pltpu.VMEM((2, 3 * cps, pair), BF16),
            pltpu.VMEM((cps, 5 * cps), F32),
            pltpu.VMEM((cps, 128), BF16),
            pltpu.VMEM((4, cps, 128), BF16),
            pltpu.VMEM((3, nz, nm, nc, cps // 2, 128), BF16),
            pltpu.VMEM((2, nz, 8, 128), F32),
            pltpu.VMEM((2, nm, 8, 128), F32),
            pltpu.VMEM((2, nc, 8, 128), F32),
            pltpu.SemaphoreType.DMA((5,)),
            pltpu.SemaphoreType.DMA((copies,)),
            pltpu.SemaphoreType.DMA((copies,)),
        ],
        compiler_params=pltpu.CompilerParams(
            collective_id=0, has_side_effects=True, vmem_limit_bytes=60 * 1024 * 1024
        ),
    )(
        lead_side.reshape(2),
        sources.reshape(2 * here, trace),
        impedance.reshape(2 * trace, trace),
        pair_maps.reshape(4, pair, pair),
        coarse_basis[0, 0],
        coarse_inverse,
    )
    return out.reshape(1, 1, 2, here, trace)


SHAPE = (8, 2, 4, 2, 2)


def build(mesh, shape):
    return jax.shard_map(
        functools.partial(per_device, shape),
        mesh=mesh,
        in_specs=(
            P("gx", "gy", None, "col", None),
            P("gx", "gy", None, None, None),
            P("gx", "gy", None, None, None, None),
            P("gx", "gy", None),
            P("gx", "gy", None, None, None),
            P(("gx", "gy", "col"), None),
        ),
        out_specs=P("gx", "gy", None, "col", None),
        check_vma=False,
    )


def solution(mesh):
    return build(mesh, SHAPE)
```

```python
import functools

import jax
import jax.numpy as jnp
from jax import lax
from jax.experimental import pallas as pl
from jax.experimental.pallas import tpu as pltpu
from jax.sharding import PartitionSpec as P

STEP_RATIO = 0.4
MESH = pl.DeviceIdType.MESH
F32 = jnp.float32
BF16 = jnp.bfloat16
HIGHEST = lax.Precision.HIGHEST


def dot(a, b, precision=None):
    return jnp.dot(a, b, preferred_element_type=F32, precision=precision)


def dot_nt(a, b, precision=None):
    return lax.dot_general(
        a, b, (((1,), (1,)), ((), ())), preferred_element_type=F32, precision=precision
    )


def dot_tn(a, b):
    return lax.dot_general(a, b, (((0,), (0,)), ((), ())), preferred_element_type=F32)


def split(x):
    high = x.astype(BF16)
    return high, (x - high.astype(F32)).astype(BF16)


def kernel(
    shape,
    lead_ref,
    src_hbm,
    imp_hbm,
    maps_hbm,
    basis_hbm,
    inv_hbm,
    out_ref,
    src,
    imp,
    maps,
    basis,
    inv,
    solver,
    inv_all,
    outgoing,
    image_out,
    face_in,
    image_in,
    ret_out,
    ret_in,
    solved_own,
    updated,
    state,
    rows,
    rows_turned,
    product,
    image,
    image_solved,
    proj_rows,
    basis_k,
    mapped,
    mapped_near,
    mapped_k,
    mapped_end,
    kernel_t,
    near_out,
    near_in,
    gathered,
    sum_z,
    sum_q,
    load_sem,
    send_sem,
    recv_sem,
):
    nz, nh, ny, nc, ncol = shape
    nm = nh * ny
    ngx, ngy = nz * nh, ny * nc
    sources = src.shape[0] // 2
    trace = src.shape[1]
    face = trace // 6
    pair = 2 * face
    cps = basis.shape[0]
    half = cps // 2

    gx, gy, col = lax.axis_index("gx"), lax.axis_index("gy"), lax.axis_index("col")
    z, xh = gx // nh, gx % nh
    y, core = gy // nc, gy % nc
    m = xh * ny + y

    def at(z_to, m_to, core_to):
        return {
            "gx": z_to * nh + m_to // ny,
            "gy": (m_to % ny) * nc + core_to,
            "col": col,
        }

    z_peers = [at((z + o) % nz, m, core) for o in range(1, nz)]
    m_peers = [at(z, (m + o) % nm, core) for o in range(1, nm)]
    c_peers = [at(z, m, (core + o) % nc) for o in range(1, nc)]
    q, nq = m * nc + core, nm * nc
    q_peers = [at(z, (q + o) % nq // nc, (q + o) % nq % nc) for o in range(1, nq)]
    offsets = [0]
    for o in range(1, nz // 2 + 1):
        offsets += [o] if 2 * o == nz else [o, nz - o]
    bounds = [0, 1] + list(range(3, nz - 2, 2)) + ([nz] if nz > 1 else [])
    groups = list(zip(bounds, bounds[1:]))
    below = [
        {"gx": (gx + ngx - 1) % ngx, "gy": gy, "col": col},
        {"gx": gx, "gy": (gy + ngy - 1) % ngy, "col": col},
    ]
    above = [
        {"gx": (gx + 1) % ngx, "gy": gy, "col": col},
        {"gx": gx, "gy": (gy + 1) % ngy, "col": col},
    ]
    col_peer = {"gx": gx, "gy": gy, "col": (col + 1) % ncol}
    position, last = [gx, gy], [ngx - 1, ngy - 1]

    loads = [
        pltpu.make_async_copy(a, b, load_sem.at[i])
        for i, (a, b) in enumerate(
            [(src_hbm, src), (maps_hbm, maps), (basis_hbm, basis), (inv_hbm, inv), (imp_hbm, imp)]
        )
    ]
    loads[0].start()

    barrier = pltpu.get_barrier_semaphore()
    partners = below + above + z_peers + q_peers + [col_peer]
    for partner in partners:
        pl.semaphore_signal(barrier, inc=1, device_id=partner, device_id_type=MESH)
    for i in (3, 1, 2, 4):
        loads[i].start()

    sent = []

    def remote(source, target, device):
        k = len(sent)
        copy = pltpu.make_async_remote_copy(
            src_ref=source,
            dst_ref=target,
            send_sem=send_sem.at[k],
            recv_sem=recv_sem.at[k],
            device_id=device,
            device_id_type=MESH,
        )
        copy.start()
        sent.append(copy)
        return copy

    def arrive(copies):
        for copy in copies:
            copy.wait_recv()

    def lanes(n):
        return lax.broadcasted_iota(jnp.int32, (n, 128), 1)

    def turned(x):
        part = x.shape[0] // 2
        return jnp.concatenate([-x[part:], x[:part]], axis=0)

    def send_faces(it):
        return [
            remote(outgoing.at[it, :, pl.ds(d * pair, 256)], face_in.at[it, d], below[d])
            for d in range(2)
        ]

    def solve(it, d, coming):
        coming[d].wait_recv()
        upper = face_in[it, d]
        here = outgoing[it, :, pl.ds(d * pair, pair)]
        middle = jnp.where(
            lanes(2 * sources) < 64, upper[:, 128:].astype(F32), here[:, 128:256].astype(F32)
        ).astype(BF16)
        x = jnp.concatenate([upper[:, :128], middle, here[:, 256:]], axis=1)
        solved = dot(x, solver[d, 0]) + dot(turned(x), solver[d, 1])
        ret_out[it, d] = solved[:, :256].astype(BF16)
        solved_own[d] = solved[:, 128:]
        return remote(ret_out.at[it, d], ret_in.at[it, d], above[d])

    def assemble(it, returned):
        ends = outgoing[it, :, pl.ds(2 * pair, pair)].astype(F32)
        updated[it, :, pl.ds(2 * pair, pair)] = pltpu.roll(ends, face, 1)
        for d in range(2):
            returned[d].wait_recv()
            back = jnp.where(position[d] > 0, ret_in[it, d].astype(F32), 0.0)
            own = jnp.where(position[d] < last[d], solved_own[d], 0.0)
            updated[it, :, pl.ds(d * pair, 128)] = back[:, :128]
            updated[it, :, pl.ds(d * pair + 128, 128)] = jnp.where(
                lanes(2 * sources) < 64, back[:, 128:], own[:, :128]
            )
            updated[it, :, pl.ds(d * pair + 256, 128)] = own[:, 128:]

    def apply_map(j):
        span = pl.ds(384 * j, 384)
        return dot(rows[...], imp[pl.ds(0, trace), span]) + dot(
            rows_turned[...], imp[pl.ds(trace, trace), span]
        )

    def packed(total):
        return jnp.where(
            lanes(half) < 64, total[:half], pltpu.roll(total[half:], sources, 1)
        ).astype(BF16)

    def project(defect):
        high, low = split(defect)
        first = dot_nt(proj_rows[...], high)
        second = dot_nt(proj_rows[pl.ds(0, 2 * cps), :], low)
        by_part = first[: 2 * cps] + first[2 * cps :] + second
        return packed(by_part[:cps] + pltpu.roll(by_part[cps:], sources, 1))

    def source_sums(products):
        folded = products[:, :128]
        for t in range(1, trace // 128):
            folded = folded + products[:, 128 * t : 128 * (t + 1)]
        folded = folded[:sources] + folded[sources:]
        both = jnp.concatenate([folded, folded], axis=0)
        return dot_nt(jnp.ones((8, 128), F32), both, HIGHEST)

    def forward(it, low, high):
        block = gathered.at[it, pl.ds(low, high - low), m, core]
        return [remote(block, block, peer) for peer in m_peers]

    def gather_start(it, block):
        gathered[it, 0, m, core] = block
        own = gathered.at[it, 0, m, core]
        coming = [None]
        for i in range(1, nz):
            coming.append(remote(own, gathered.at[it, i, m, core], z_peers[offsets[i] - 1]))
        return coming

    def gather_group(it, coming, low, high):
        arrive(coming[max(low, 1) : high])
        return forward(it, low, high)

    def gather_core(it, coming, low, high):
        arrive(coming)
        block = gathered.at[it, pl.ds(low, high - low), :, core]
        return [remote(block, block, peer) for peer in c_peers]

    def coarse_of(it, coming):
        arrive(coming)
        parts = 0.0
        for i in range(nz):
            parts = parts + dot(
                inv_all[i].reshape(2 * cps, nq * half), gathered[it, i].reshape(nq * half, 128)
            )
        return parts[:cps] + pltpu.roll(parts[cps:], sources, 1)

    def share(buffer, it, index, peers, row):
        buffer[it, index] = row
        own = buffer.at[it, index]
        return [remote(own, own, peer) for peer in peers]

    def added(buffer, it, coming):
        arrive(coming)
        row = buffer[it, 0]
        for i in range(1, buffer.shape[1]):
            row = row + buffer[it, i]
        return row

    def stacked(coefficients):
        high, low = split(coefficients)
        return jnp.concatenate([high, low, high], axis=0)[:, :sources]

    def factor_of(total):
        return STEP_RATIO * jnp.sqrt(total / (pltpu.roll(total, sources, 1) + 1e-06))

    def energy_of(coarse):
        energy = jnp.sum(coarse * dot(gram, coarse, HIGHEST), axis=0, keepdims=True)
        return pltpu.roll(jnp.broadcast_to(energy, (8, 128)), sources, 1)

    def three(block):
        high, low = split(block)
        return jnp.concatenate([high, high, low], axis=0)

    def mapped_sum(near, c, d):
        if d == 2:
            return dot_tn(stacked(near[0]), mapped_end[c])
        coefficients = jnp.concatenate(
            [stacked(near[0]), stacked(near[1 + 2 * d]), stacked(near[2 + 2 * d])], axis=0
        )
        return dot_tn(coefficients, mapped_k[c, d])

    loads[0].wait()
    outgoing[0] = src[...].astype(BF16)
    pl.semaphore_wait(barrier, len(partners))
    faces = send_faces(0)

    loads[3].wait()
    here = lax.broadcasted_iota(jnp.int32, (256, 256), 0)
    there = lax.broadcasted_iota(jnp.int32, (256, 256), 1)
    wanted = ((here // half) % 2) * 128 + (here // cps) * half + here % half
    order = jnp.where(there == wanted, 1.0, 0.0).astype(BF16)
    chunks = nq * cps // 256
    for i in range(nz):
        source_z = (z + nz - offsets[i]) % nz
        for j in range(chunks):
            start = pl.multiple_of((source_z * chunks + j) * 256, 256)
            moved = dot(inv[:, pl.ds(start, 256)].astype(BF16), order).astype(BF16)
            for h in range(2):
                inv_all[i, h, col, :, pl.ds(128 * j, 128)] = moved[:, 128 * h : 128 * (h + 1)]
    inverse_coming = remote(inv_all.at[:, :, col], inv_all.at[:, :, col], col_peer)
    loads[1].wait()
    for d in range(2):
        for c in range(2):
            stored = maps[2 * d + c].astype(F32)
            swapped = jnp.concatenate([stored[face:], stored[:face]], axis=0)
            swapped = pltpu.roll(swapped, face, 1)
            solver[d, c] = jnp.where(lead_ref[d] == 0, swapped, stored).astype(BF16)
    loads[2].wait()
    both = jnp.concatenate([basis[:, 0, :], basis[:, 1, :]], axis=0)
    high, low = split(both)
    proj_rows[pl.ds(0, 2 * cps), :] = high
    proj_rows[pl.ds(2 * cps, 2 * cps), :] = low
    for part, block in enumerate((high, low)):
        rows[pl.ds(part * 2 * cps, 2 * cps), :] = block
        rows_turned[pl.ds(part * 2 * cps, 2 * cps), :] = turned(block)
    returned = [solve(0, d, faces) for d in range(2)]

    loads[4].wait()
    for j in range(trace // 384):
        whole = apply_map(j)
        whole = whole[: 2 * cps] + whole[2 * cps :]
        image[:, pl.ds(384 * j, 384)] = whole
        image_out[:, pl.ds(384 * j, 384)] = whole.astype(BF16)
    assemble(0, returned)

    coming = gather_start(0, project(updated[0]))
    moving = [gather_group(0, coming, *groups[0])]
    image_coming = [
        remote(image_out.at[:, pl.ds(d * pair, 256)], image_in.at[d], below[d]) for d in range(2)
    ]
    high = updated[0].astype(BF16)
    rows[...] = high
    rows_turned[...] = turned(high)
    for j in range(trace // 384):
        span = pl.ds(384 * j, 384)
        outgoing[1, :, span] = (apply_map(j) + src[:, span]).astype(BF16)
        if j + 1 < len(groups):
            moving.append(gather_group(0, coming, *groups[j + 1]))
    faces_next = send_faces(1)

    image_returned = []
    for d in range(2):
        image_coming[d].wait_recv()
        upper = image_in[d].astype(F32)
        own = image_out[:, pl.ds(d * pair, pair)].astype(F32)
        low_lane = lanes(2 * cps) < 64
        zero = jnp.zeros((2 * cps, 128), F32)
        x = jnp.concatenate(
            [zero, jnp.where(low_lane, 0.0, own[:, 128:256]), own[:, 256:]], axis=1
        ).astype(BF16)
        w = jnp.concatenate(
            [upper[:, :128], jnp.where(low_lane, upper[:, 128:], 0.0), zero], axis=1
        ).astype(BF16)
        solved = dot(jnp.concatenate([x, w], axis=0), solver[d, 0]) + dot(
            jnp.concatenate([turned(x), turned(w)], axis=0), solver[d, 1]
        )
        ret_out[2, d] = solved[:, :256].astype(BF16)
        image_solved[d] = solved[:, 128:]
        image_returned.append(remote(ret_out.at[2, d], ret_in.at[2, d], above[d]))
    first_squares = source_sums(updated[0] * updated[0])
    gram = dot_nt(both[:cps], both[:cps], HIGHEST) + dot_nt(both[cps:], both[cps:], HIGHEST)
    for c in range(2):
        basis_k[c] = three(both[c * cps : (c + 1) * cps])
    split_at = groups[-1][0]
    coming = gather_core(0, sum(moving[:-1], []), 0, split_at)
    returned = [solve(1, d, faces_next) for d in range(2)]
    coming += gather_core(0, moving[-1], split_at, nz)

    inverse_coming.wait_recv()
    coarse = coarse_of(0, coming)
    high, low = split(coarse)
    near_out[...] = jnp.where(
        lanes(cps) < 64, high.astype(F32), pltpu.roll(low.astype(F32), sources, 1)
    ).astype(BF16)
    near_coming = []
    for d in range(2):
        near_coming.append(remote(near_out, near_in.at[2 * d], above[d]))
        near_coming.append(remote(near_out, near_in.at[2 * d + 1], below[d]))
    first_row = jnp.where(lanes(8) < 64, first_squares, energy_of(coarse))

    assemble(1, returned)
    state[...] = updated[1] - updated[0]
    early = gather_start(2, project(state[...]))
    for d in range(2):
        image_returned[d].wait_recv()
        back = jnp.where(position[d] > 0, ret_in[2, d].astype(F32), 0.0)
        own = jnp.where(position[d] < last[d], image_solved[d], 0.0)
        for target, r, o in ((mapped, 2 * cps, 0), (mapped_near, 0, 2 * cps)):
            target[:, pl.ds(d * pair, 128)] = back[r : r + 2 * cps, :128]
            target[:, pl.ds(d * pair + 128, 128)] = jnp.where(
                lanes(2 * cps) < 64, back[r : r + 2 * cps, 128:], own[o : o + 2 * cps, :128]
            )
            target[:, pl.ds(d * pair + 256, 128)] = own[o : o + 2 * cps, 128:]
    mapped[:, pl.ds(2 * pair, pair)] = pltpu.roll(image[:, pl.ds(2 * pair, pair)], face, 1)
    moved = mapped[...] - both
    blocks = [
        dot_nt(moved[:cps], both[:cps], HIGHEST) + dot_nt(moved[cps:], both[cps:], HIGHEST)
    ]
    left = lax.broadcasted_iota(jnp.int32, (cps, pair), 1) < face
    for d in range(2):
        total = 0.0
        for c in range(2):
            part = mapped_near[pl.ds(c * cps, cps), pl.ds(d * pair, pair)]
            sides = jnp.concatenate([jnp.where(left, part, 0.0), jnp.where(left, 0.0, part)], axis=0)
            total = total + dot_nt(
                sides, both[c * cps : (c + 1) * cps, d * pair : (d + 1) * pair], HIGHEST
            )
            own = three(mapped[pl.ds(c * cps, cps), pl.ds(d * pair, pair)])
            mapped_k[c, d] = jnp.concatenate(
                [own, three(sides[:cps]), three(sides[cps:])], axis=0
            )
        blocks.append(total)
    for c in range(2):
        mapped_end[c] = three(mapped[pl.ds(c * cps, cps), pl.ds(2 * pair, pair)])
    kernel_t[...] = jnp.concatenate(blocks, axis=0).T

    arrive(near_coming)
    near = [coarse]
    for i in range(4):
        both_parts = near_in[i].astype(F32)
        near.append(both_parts + pltpu.roll(both_parts, sources, 1))
    coming = gather_start(
        1, packed(dot(kernel_t[...], jnp.concatenate(near, axis=0), HIGHEST))
    )
    norms = share(sum_z, 0, z, z_peers, first_row)
    moving = [gather_group(1, coming, *groups[0])]
    early = gather_group(2, early, 0, nz)
    for c in range(2):
        part = pl.ds(c * sources, sources)
        for d in range(3):
            product[part, pl.ds(d * pair, pair)] = mapped_sum(near, c, d)
        product[part, :] = product[part, :] - dot_tn(stacked(coarse), basis_k[c])
        if c + 1 < len(groups):
            moving.append(gather_group(1, coming, *groups[c + 1]))
    for group in groups[3:]:
        moving.append(gather_group(1, coming, *group))
    norms = share(sum_q, 0, q, q_peers, added(sum_z, 0, norms))
    sums_aa = source_sums(state[...] * state[...])
    sums_ab = source_sums(state[...] * product[...])
    sums_bb = source_sums(product[...] * product[...])
    early = gather_core(2, early, 0, nz)
    late = gather_core(1, sum(moving[:-1], []), 0, split_at)
    coarse_early = coarse_of(2, early)
    late += gather_core(1, moving[-1], split_at, nz)
    factor = factor_of(added(sum_q, 0, norms))
    coarse = coarse_early + factor[0:1] * coarse_of(1, late)
    squares = sums_aa + factor * (2.0 * sums_ab + factor * sums_bb)
    row = jnp.where(lanes(8) < 64, squares, energy_of(coarse))
    norms = share(sum_z, 1, z, z_peers, row)
    near = [factor[0:1] * part for part in near]
    for c in range(2):
        part = pl.ds(c * sources, sources)
        for d in range(3):
            span = pl.ds(d * pair, pair)
            updated[1, part, span] = updated[1, part, span] + mapped_sum(near, c, d)
    norms = share(sum_q, 1, q, q_peers, added(sum_z, 1, norms))
    factor = factor_of(added(sum_q, 1, norms))
    scaled = stacked(factor[0:1] * coarse)
    for c in range(2):
        part = pl.ds(c * sources, sources)
        out_ref[part, :] = updated[1, part, :] + dot_tn(scaled, basis_k[c])
    for copy in sent:
        copy.wait_send()


def per_device(shape, sources, impedance, pair_maps, lead_side, coarse_basis, coarse_inverse):
    nz, nh, ny, nc, ncol = shape
    here, trace = sources.shape[3], sources.shape[4]
    pair = pair_maps.shape[-1]
    cps = coarse_basis.shape[2]
    size = coarse_inverse.shape[1]
    nm = nh * ny
    copies = 1 + 3 * 4 + 4 + 3 * (nz - 1) + 9 * (nm - 1) + 5 * (nc - 1)
    copies += 2 * (nz - 1 + nm * nc - 1)
    hbm = pl.BlockSpec(memory_space=pltpu.HBM)
    out = pl.pallas_call(
        functools.partial(kernel, shape),
        out_shape=jax.ShapeDtypeStruct((2 * here, trace), F32),
        in_specs=[pl.BlockSpec(memory_space=pltpu.SMEM)] + [hbm] * 5,
        out_specs=pl.BlockSpec(memory_space=pltpu.VMEM),
        scratch_shapes=[
            pltpu.VMEM((2 * here, trace), F32),
            pltpu.VMEM((2 * trace, trace), BF16),
            pltpu.VMEM((4, pair, pair), BF16),
            pltpu.VMEM((cps, 2, trace), F32),
            pltpu.VMEM((cps // 2, size), F32),
            pltpu.VMEM((2, 2, pair, pair), BF16),
            pltpu.VMEM((nz, 2, ncol, cps // 2, nm * nc * cps // 2), BF16),
            pltpu.VMEM((2, 2 * here, trace), BF16),
            pltpu.VMEM((2 * cps, trace), BF16),
            pltpu.VMEM((2, 2, 2 * here, 256), BF16),
            pltpu.VMEM((2, 2 * cps, 256), BF16),
            pltpu.VMEM((3, 2, 2 * here, 256), BF16),
            pltpu.VMEM((3, 2, 2 * here, 256), BF16),
            pltpu.VMEM((2, 2 * here, 256), F32),
            pltpu.VMEM((2, 2 * here, trace), F32),
            pltpu.VMEM((2 * here, trace), F32),
            pltpu.VMEM((2 * here, trace), BF16),
            pltpu.VMEM((2 * here, trace), BF16),
            pltpu.VMEM((2 * here, trace), F32),
            pltpu.VMEM((2 * cps, trace), F32),
            pltpu.VMEM((2, 4 * cps, 256), F32),
            pltpu.VMEM((4 * cps, trace), BF16),
            pltpu.VMEM((2, 3 * cps, trace), BF16),
            pltpu.VMEM((2 * cps, trace), F32),
            pltpu.VMEM((2 * cps, 2 * pair), F32),
            pltpu.VMEM((2, 2, 9 * cps, pair), BF16),
            pltpu.VMEM((2, 3 * cps, pair), BF16),
            pltpu.VMEM((cps, 5 * cps), F32),
            pltpu.VMEM((cps, 128), BF16),
            pltpu.VMEM((4, cps, 128), BF16),
            pltpu.VMEM((3, nz, nm, nc, cps // 2, 128), BF16),
            pltpu.VMEM((2, nz, 8, 128), F32),
            pltpu.VMEM((2, nm * nc, 8, 128), F32),
            pltpu.SemaphoreType.DMA((5,)),
            pltpu.SemaphoreType.DMA((copies,)),
            pltpu.SemaphoreType.DMA((copies,)),
        ],
        compiler_params=pltpu.CompilerParams(
            collective_id=0, has_side_effects=True, vmem_limit_bytes=60 * 1024 * 1024
        ),
    )(
        lead_side.reshape(2),
        sources.reshape(2 * here, trace),
        impedance.reshape(2 * trace, trace),
        pair_maps.reshape(4, pair, pair),
        coarse_basis[0, 0],
        coarse_inverse,
    )
    return out.reshape(1, 1, 2, here, trace)


SHAPE = (8, 2, 4, 2, 2)


def build(mesh, shape):
    return jax.shard_map(
        functools.partial(per_device, shape),
        mesh=mesh,
        in_specs=(
            P("gx", "gy", None, "col", None),
            P("gx", "gy", None, None, None),
            P("gx", "gy", None, None, None, None),
            P("gx", "gy", None),
            P("gx", "gy", None, None, None),
            P(("gx", "gy", "col"), None),
        ),
        out_specs=P("gx", "gy", None, "col", None),
        check_vma=False,
    )


def solution(mesh):
    return build(mesh, SHAPE)
```

```python
import functools

import jax
import jax.numpy as jnp
from jax import lax
from jax.experimental import pallas as pl
from jax.experimental.pallas import tpu as pltpu
from jax.sharding import PartitionSpec as P

STEP_RATIO = 0.4
MESH = pl.DeviceIdType.MESH
F32 = jnp.float32
BF16 = jnp.bfloat16
HIGHEST = lax.Precision.HIGHEST


def dot(a, b, precision=None):
    return jnp.dot(a, b, preferred_element_type=F32, precision=precision)


def dot_nt(a, b, precision=None):
    return lax.dot_general(
        a, b, (((1,), (1,)), ((), ())), preferred_element_type=F32, precision=precision
    )


def dot_tn(a, b):
    return lax.dot_general(a, b, (((0,), (0,)), ((), ())), preferred_element_type=F32)


def split(x):
    high = x.astype(BF16)
    return high, (x - high.astype(F32)).astype(BF16)


def kernel(
    shape,
    lead_ref,
    src_hbm,
    imp_hbm,
    maps_hbm,
    basis_hbm,
    inv_hbm,
    out_ref,
    src,
    imp,
    maps,
    basis,
    inv,
    solver,
    inv_all,
    outgoing,
    image_out,
    face_out,
    face_in,
    image_in,
    ret_out,
    ret_in,
    solved_own,
    updated,
    state,
    rows,
    rows_turned,
    product,
    image,
    image_solved,
    proj_rows,
    basis_k,
    mapped,
    mapped_near,
    mapped_k,
    mapped_end,
    kernel_t,
    near_out,
    near_in,
    gathered,
    sum_z,
    sum_q,
    load_sem,
    send_sem,
    recv_sem,
):
    nz, nh, ny, nc, ncol = shape
    nm = nh * ny
    ngx, ngy = nz * nh, ny * nc
    sources = src.shape[0] // 2
    trace = src.shape[1]
    face = trace // 6
    pair = 2 * face
    cps = basis.shape[0]
    half = cps // 2

    gx, gy, col = lax.axis_index("gx"), lax.axis_index("gy"), lax.axis_index("col")
    z, xh = gx // nh, gx % nh
    y, core = gy // nc, gy % nc
    m = xh * ny + y

    def at(z_to, m_to, core_to):
        return {
            "gx": z_to * nh + m_to // ny,
            "gy": (m_to % ny) * nc + core_to,
            "col": col,
        }

    z_peers = [at((z + o) % nz, m, core) for o in range(1, nz)]
    m_peers = [at(z, (m + o) % nm, core) for o in range(1, nm)]
    c_peers = [at(z, m, (core + o) % nc) for o in range(1, nc)]
    q, nq = m * nc + core, nm * nc
    q_peers = [at(z, (q + o) % nq // nc, (q + o) % nq % nc) for o in range(1, nq)]
    offsets = [0]
    for o in range(1, nz // 2 + 1):
        offsets += [o] if 2 * o == nz else [o, nz - o]
    bounds = [0, 1] + list(range(3, nz - 2, 2)) + ([nz] if nz > 1 else [])
    groups = list(zip(bounds, bounds[1:]))
    below = [
        {"gx": (gx + ngx - 1) % ngx, "gy": gy, "col": col},
        {"gx": gx, "gy": (gy + ngy - 1) % ngy, "col": col},
    ]
    above = [
        {"gx": (gx + 1) % ngx, "gy": gy, "col": col},
        {"gx": gx, "gy": (gy + 1) % ngy, "col": col},
    ]
    col_peer = {"gx": gx, "gy": gy, "col": (col + 1) % ncol}
    position, last = [gx, gy], [ngx - 1, ngy - 1]

    loads = [
        pltpu.make_async_copy(a, b, load_sem.at[i])
        for i, (a, b) in enumerate(
            [(src_hbm, src), (maps_hbm, maps), (basis_hbm, basis), (inv_hbm, inv), (imp_hbm, imp)]
        )
    ]
    loads[0].start()

    barrier = pltpu.get_barrier_semaphore()
    partners = below + above + z_peers + q_peers + [col_peer]
    for partner in partners:
        pl.semaphore_signal(barrier, inc=1, device_id=partner, device_id_type=MESH)
    for i in (3, 1, 2, 4):
        loads[i].start()

    sent = []

    def remote(source, target, device):
        k = len(sent)
        copy = pltpu.make_async_remote_copy(
            src_ref=source,
            dst_ref=target,
            send_sem=send_sem.at[k],
            recv_sem=recv_sem.at[k],
            device_id=device,
            device_id_type=MESH,
        )
        copy.start()
        sent.append(copy)
        return copy

    def arrive(copies):
        for copy in copies:
            copy.wait_recv()

    def lanes(n):
        return lax.broadcasted_iota(jnp.int32, (n, 128), 1)

    def turned(x):
        part = x.shape[0] // 2
        return jnp.concatenate([-x[part:], x[:part]], axis=0)

    def packed_face(x):
        part = x.shape[0] // 2
        tail = jnp.where(
            lanes(part) < 64, x[:part, 128:256], pltpu.roll(x[part:, 128:256], 64, 1)
        )
        return jnp.concatenate([x[:, :128], tail], axis=0).astype(BF16)

    def face_parts(x):
        size = 2 * x.shape[0] // 3
        tail = x[size:].astype(F32)
        return x[:size].astype(F32), jnp.concatenate([tail, pltpu.roll(tail, 64, 1)], axis=0)

    def send_face(it, d):
        face_out[it, d] = packed_face(outgoing[it, :, pl.ds(d * pair, 256)].astype(F32))
        return remote(face_out.at[it, d], face_in.at[it, d], below[d])

    def solve(it, d, coming):
        coming[d].wait_recv()
        head, tail = face_parts(face_in[it, d])
        here = outgoing[it, :, pl.ds(d * pair, pair)]
        middle = jnp.where(lanes(2 * sources) < 64, tail, here[:, 128:256].astype(F32))
        x = jnp.concatenate([head.astype(BF16), middle.astype(BF16), here[:, 256:]], axis=1)
        solved = dot(x, solver[d, 0]) + dot(turned(x), solver[d, 1])
        ret_out[it, d] = packed_face(solved)
        solved_own[d] = solved[:, 128:]
        return remote(ret_out.at[it, d], ret_in.at[it, d], above[d])

    def assemble(it, returned):
        ends = outgoing[it, :, pl.ds(2 * pair, pair)].astype(F32)
        updated[it, :, pl.ds(2 * pair, pair)] = pltpu.roll(ends, face, 1)
        for d in range(2):
            returned[d].wait_recv()
            head, tail = face_parts(ret_in[it, d])
            own = jnp.where(position[d] < last[d], solved_own[d], 0.0)
            updated[it, :, pl.ds(d * pair, 128)] = jnp.where(position[d] > 0, head, 0.0)
            updated[it, :, pl.ds(d * pair + 128, 128)] = jnp.where(
                lanes(2 * sources) < 64, jnp.where(position[d] > 0, tail, 0.0), own[:, :128]
            )
            updated[it, :, pl.ds(d * pair + 256, 128)] = own[:, 128:]

    def apply_map(j):
        span = pl.ds(384 * j, 384)
        return dot(rows[...], imp[pl.ds(0, trace), span]) + dot(
            rows_turned[...], imp[pl.ds(trace, trace), span]
        )

    def packed(total):
        return jnp.where(
            lanes(half) < 64, total[:half], pltpu.roll(total[half:], sources, 1)
        ).astype(BF16)

    def project(defect):
        high, low = split(defect)
        first = dot_nt(proj_rows[...], high)
        second = dot_nt(proj_rows[pl.ds(0, 2 * cps), :], low)
        by_part = first[: 2 * cps] + first[2 * cps :] + second
        return packed(by_part[:cps] + pltpu.roll(by_part[cps:], sources, 1))

    def source_sums(products):
        folded = products[:, :128]
        for t in range(1, trace // 128):
            folded = folded + products[:, 128 * t : 128 * (t + 1)]
        folded = folded[:sources] + folded[sources:]
        both = jnp.concatenate([folded, folded], axis=0)
        return dot_nt(jnp.ones((8, 128), F32), both, HIGHEST)

    def forward(it, low, high):
        block = gathered.at[it, pl.ds(low, high - low), m, core]
        return [remote(block, block, peer) for peer in m_peers]

    def gather_start(it, block):
        gathered[it, 0, m, core] = block
        own = gathered.at[it, 0, m, core]
        coming = [None]
        for i in range(1, nz):
            coming.append(remote(own, gathered.at[it, i, m, core], z_peers[offsets[i] - 1]))
        return coming

    def gather_group(it, coming, low, high):
        arrive(coming[max(low, 1) : high])
        return forward(it, low, high)

    def gather_core(it, coming, low, high):
        arrive(coming)
        block = gathered.at[it, pl.ds(low, high - low), :, core]
        return [remote(block, block, peer) for peer in c_peers]

    def coarse_of(it, coming):
        arrive(coming)
        parts = 0.0
        for i in range(nz):
            parts = parts + dot(
                inv_all[i].reshape(2 * cps, nq * half), gathered[it, i].reshape(nq * half, 128)
            )
        return parts[:cps] + pltpu.roll(parts[cps:], sources, 1)

    def share(buffer, it, index, peers, row):
        buffer[it, index] = row[0:1]
        own = buffer.at[it, index]
        return [remote(own, own, peer) for peer in peers]

    def added(buffer, it, coming):
        arrive(coming)
        row = buffer[it, 0]
        for i in range(1, buffer.shape[1]):
            row = row + buffer[it, i]
        return jnp.broadcast_to(row, (8, 128))

    def stacked(coefficients):
        high, low = split(coefficients)
        return jnp.concatenate([high, low, high], axis=0)[:, :sources]

    def factor_of(total):
        return STEP_RATIO * jnp.sqrt(total / (pltpu.roll(total, sources, 1) + 1e-06))

    def energy_of(coarse):
        energy = jnp.sum(coarse * dot(gram, coarse, HIGHEST), axis=0, keepdims=True)
        return pltpu.roll(jnp.broadcast_to(energy, (8, 128)), sources, 1)

    def three(block):
        high, low = split(block)
        return jnp.concatenate([high, high, low], axis=0)

    def mapped_sum(near, c, d):
        if d == 2:
            return dot_tn(stacked(near[0]), mapped_end[c])
        coefficients = jnp.concatenate(
            [stacked(near[0]), stacked(near[1 + 2 * d]), stacked(near[2 + 2 * d])], axis=0
        )
        return dot_tn(coefficients, mapped_k[c, d])

    loads[0].wait()
    outgoing[0] = src[...].astype(BF16)
    pl.semaphore_wait(barrier, len(partners))
    faces = [send_face(0, d) for d in range(2)]

    loads[2].wait()
    both = jnp.concatenate([basis[:, 0, :], basis[:, 1, :]], axis=0)
    high, low = split(both)
    proj_rows[pl.ds(0, 2 * cps), :] = high
    proj_rows[pl.ds(2 * cps, 2 * cps), :] = low
    for part, block in enumerate((high, low)):
        rows[pl.ds(part * 2 * cps, 2 * cps), :] = block
        rows_turned[pl.ds(part * 2 * cps, 2 * cps), :] = turned(block)

    loads[4].wait()

    def apply_to_basis(j):
        whole = apply_map(j)
        whole = whole[: 2 * cps] + whole[2 * cps :]
        image[:, pl.ds(384 * j, 384)] = whole
        return whole

    image_coming = []
    for j in range(2):
        image_out[j] = packed_face(apply_to_basis(j))
        image_coming.append(remote(image_out.at[j], image_in.at[j], below[j]))
    loads[1].wait()
    for d in range(2):
        for c in range(2):
            stored = maps[2 * d + c].astype(F32)
            swapped = jnp.concatenate([stored[face:], stored[:face]], axis=0)
            swapped = pltpu.roll(swapped, face, 1)
            solver[d, c] = jnp.where(lead_ref[d] == 0, swapped, stored).astype(BF16)
    returned = [solve(0, d, faces) for d in range(2)]
    apply_to_basis(2)

    loads[3].wait()
    here = lax.broadcasted_iota(jnp.int32, (256, 256), 0)
    there = lax.broadcasted_iota(jnp.int32, (256, 256), 1)
    wanted = ((here // half) % 2) * 128 + (here // cps) * half + here % half
    order = jnp.where(there == wanted, 1.0, 0.0).astype(BF16)
    chunks = nq * cps // 256
    for i in range(nz):
        source_z = (z + nz - offsets[i]) % nz
        for j in range(chunks):
            start = pl.multiple_of((source_z * chunks + j) * 256, 256)
            moved = dot(inv[:, pl.ds(start, 256)].astype(BF16), order).astype(BF16)
            for h in range(2):
                inv_all[i, h, col, :, pl.ds(128 * j, 128)] = moved[:, 128 * h : 128 * (h + 1)]

    image_returned = []
    for d in range(2):
        image_coming[d].wait_recv()
        head, tail = face_parts(image_in[d])
        own = image[:, pl.ds(d * pair, pair)]
        low_lane = lanes(2 * cps) < 64
        zero = jnp.zeros((2 * cps, 128), F32)
        x = jnp.concatenate(
            [zero, jnp.where(low_lane, 0.0, own[:, 128:256]), own[:, 256:]], axis=1
        ).astype(BF16)
        w = jnp.concatenate(
            [head, jnp.where(low_lane, tail, 0.0), zero], axis=1
        ).astype(BF16)
        solved = dot(jnp.concatenate([x, w], axis=0), solver[d, 0]) + dot(
            jnp.concatenate([turned(x), turned(w)], axis=0), solver[d, 1]
        )
        ret_out[2, d] = packed_face(solved)
        image_solved[d] = solved[:, 128:]
        image_returned.append(remote(ret_out.at[2, d], ret_in.at[2, d], above[d]))
    gram = dot_nt(both[:cps], both[:cps], HIGHEST) + dot_nt(both[cps:], both[cps:], HIGHEST)
    for c in range(2):
        basis_k[c] = three(both[c * cps : (c + 1) * cps])
    assemble(0, returned)

    coming = gather_start(0, project(updated[0]))
    inverse_coming = remote(inv_all.at[:, :, col], inv_all.at[:, :, col], col_peer)
    moving = [gather_group(0, coming, *groups[0])]
    high = updated[0].astype(BF16)
    rows[...] = high
    rows_turned[...] = turned(high)
    faces_next = []
    for j in range(trace // 384):
        span = pl.ds(384 * j, 384)
        outgoing[1, :, span] = (apply_map(j) + src[:, span]).astype(BF16)
        if j < 2:
            faces_next.append(send_face(1, j))
        if j + 1 < len(groups):
            moving.append(gather_group(0, coming, *groups[j + 1]))

    first_squares = source_sums(updated[0] * updated[0])
    for d in range(2):
        image_returned[d].wait_recv()
        back = jnp.concatenate(face_parts(ret_in[2, d]), axis=1)
        back = jnp.where(position[d] > 0, back, 0.0)
        own = jnp.where(position[d] < last[d], image_solved[d], 0.0)
        for target, r, o in ((mapped, 2 * cps, 0), (mapped_near, 0, 2 * cps)):
            target[:, pl.ds(d * pair, 128)] = back[r : r + 2 * cps, :128]
            target[:, pl.ds(d * pair + 128, 128)] = jnp.where(
                lanes(2 * cps) < 64, back[r : r + 2 * cps, 128:], own[o : o + 2 * cps, :128]
            )
            target[:, pl.ds(d * pair + 256, 128)] = own[o : o + 2 * cps, 128:]
    mapped[:, pl.ds(2 * pair, pair)] = pltpu.roll(image[:, pl.ds(2 * pair, pair)], face, 1)
    moved = mapped[...] - both
    blocks = [
        dot_nt(moved[:cps], both[:cps], HIGHEST) + dot_nt(moved[cps:], both[cps:], HIGHEST)
    ]
    left = lax.broadcasted_iota(jnp.int32, (cps, pair), 1) < face
    for d in range(2):
        total = 0.0
        for c in range(2):
            part = mapped_near[pl.ds(c * cps, cps), pl.ds(d * pair, pair)]
            sides = jnp.concatenate([jnp.where(left, part, 0.0), jnp.where(left, 0.0, part)], axis=0)
            total = total + dot_nt(
                sides, both[c * cps : (c + 1) * cps, d * pair : (d + 1) * pair], HIGHEST
            )
            own = three(mapped[pl.ds(c * cps, cps), pl.ds(d * pair, pair)])
            mapped_k[c, d] = jnp.concatenate(
                [own, three(sides[:cps]), three(sides[cps:])], axis=0
            )
        blocks.append(total)
    for c in range(2):
        mapped_end[c] = three(mapped[pl.ds(c * cps, cps), pl.ds(2 * pair, pair)])
    kernel_t[...] = jnp.concatenate(blocks, axis=0).T

    split_at = groups[-1][0]
    coming = gather_core(0, sum(moving[:-1], []), 0, split_at)
    coming += gather_core(0, moving[-1], split_at, nz)
    returned = [solve(1, d, faces_next) for d in range(2)]

    inverse_coming.wait_recv()
    coarse = coarse_of(0, coming)
    high, low = split(coarse)
    near_out[...] = jnp.where(
        lanes(cps) < 64, high.astype(F32), pltpu.roll(low.astype(F32), sources, 1)
    ).astype(BF16)
    near_coming = []
    for d in range(2):
        near_coming.append(remote(near_out, near_in.at[2 * d], above[d]))
        near_coming.append(remote(near_out, near_in.at[2 * d + 1], below[d]))
    first_row = jnp.where(lanes(8) < 64, first_squares, energy_of(coarse))

    assemble(1, returned)
    state[...] = updated[1] - updated[0]
    early = gather_start(2, project(state[...]))

    arrive(near_coming)
    near = [coarse]
    for i in range(4):
        both_parts = near_in[i].astype(F32)
        near.append(both_parts + pltpu.roll(both_parts, sources, 1))
    coming = gather_start(
        1, packed(dot(kernel_t[...], jnp.concatenate(near, axis=0), HIGHEST))
    )
    norms = share(sum_z, 0, z, z_peers, first_row)
    moving = [gather_group(1, coming, *groups[0])]
    early = gather_group(2, early, 0, nz)
    for c in range(2):
        part = pl.ds(c * sources, sources)
        for d in range(3):
            product[part, pl.ds(d * pair, pair)] = mapped_sum(near, c, d)
        product[part, :] = product[part, :] - dot_tn(stacked(coarse), basis_k[c])
        if c + 1 < len(groups):
            moving.append(gather_group(1, coming, *groups[c + 1]))
    for group in groups[3:]:
        moving.append(gather_group(1, coming, *group))
    norms = share(sum_q, 0, q, q_peers, added(sum_z, 0, norms))
    sums_aa = source_sums(state[...] * state[...])
    sums_ab = source_sums(state[...] * product[...])
    sums_bb = source_sums(product[...] * product[...])
    early = gather_core(2, early, 0, nz)
    late = gather_core(1, sum(moving[:-1], []), 0, split_at)
    coarse_early = coarse_of(2, early)
    late += gather_core(1, moving[-1], split_at, nz)
    factor = factor_of(added(sum_q, 0, norms))
    coarse = coarse_early + factor[0:1] * coarse_of(1, late)
    squares = sums_aa + factor * (2.0 * sums_ab + factor * sums_bb)
    row = jnp.where(lanes(8) < 64, squares, energy_of(coarse))
    norms = share(sum_z, 1, z, z_peers, row)
    near = [factor[0:1] * part for part in near]
    for c in range(2):
        part = pl.ds(c * sources, sources)
        for d in range(3):
            span = pl.ds(d * pair, pair)
            updated[1, part, span] = updated[1, part, span] + mapped_sum(near, c, d)
    norms = share(sum_q, 1, q, q_peers, added(sum_z, 1, norms))
    factor = factor_of(added(sum_q, 1, norms))
    scaled = stacked(factor[0:1] * coarse)
    for c in range(2):
        part = pl.ds(c * sources, sources)
        out_ref[part, :] = updated[1, part, :] + dot_tn(scaled, basis_k[c])
    for copy in sent:
        copy.wait_send()


def per_device(shape, sources, impedance, pair_maps, lead_side, coarse_basis, coarse_inverse):
    nz, nh, ny, nc, ncol = shape
    here, trace = sources.shape[3], sources.shape[4]
    pair = pair_maps.shape[-1]
    cps = coarse_basis.shape[2]
    size = coarse_inverse.shape[1]
    nm = nh * ny
    copies = 1 + 3 * 4 + 4 + 3 * (nz - 1) + 9 * (nm - 1) + 5 * (nc - 1)
    copies += 2 * (nz - 1 + nm * nc - 1)
    def keep(array):
        return pltpu.with_memory_space_constraint(array, pltpu.HBM)

    hbm = pl.BlockSpec(memory_space=pltpu.HBM)
    out = pl.pallas_call(
        functools.partial(kernel, shape),
        out_shape=jax.ShapeDtypeStruct((2 * here, trace), F32),
        in_specs=[pl.BlockSpec(memory_space=pltpu.SMEM)] + [hbm] * 5,
        out_specs=pl.BlockSpec(memory_space=pltpu.VMEM),
        scratch_shapes=[
            pltpu.VMEM((2 * here, trace), F32),
            pltpu.VMEM((2 * trace, trace), BF16),
            pltpu.VMEM((4, pair, pair), BF16),
            pltpu.VMEM((cps, 2, trace), F32),
            pltpu.VMEM((cps // 2, size), F32),
            pltpu.VMEM((2, 2, pair, pair), BF16),
            pltpu.VMEM((nz, 2, ncol, cps // 2, nm * nc * cps // 2), BF16),
            pltpu.VMEM((2, 2 * here, trace), BF16),
            pltpu.VMEM((2, 3 * cps, 128), BF16),
            pltpu.VMEM((2, 2, 3 * here, 128), BF16),
            pltpu.VMEM((2, 2, 3 * here, 128), BF16),
            pltpu.VMEM((2, 3 * cps, 128), BF16),
            pltpu.VMEM((3, 2, 3 * here, 128), BF16),
            pltpu.VMEM((3, 2, 3 * here, 128), BF16),
            pltpu.VMEM((2, 2 * here, 256), F32),
            pltpu.VMEM((2, 2 * here, trace), F32),
            pltpu.VMEM((2 * here, trace), F32),
            pltpu.VMEM((2 * here, trace), BF16),
            pltpu.VMEM((2 * here, trace), BF16),
            pltpu.VMEM((2 * here, trace), F32),
            pltpu.VMEM((2 * cps, trace), F32),
            pltpu.VMEM((2, 4 * cps, 256), F32),
            pltpu.VMEM((4 * cps, trace), BF16),
            pltpu.VMEM((2, 3 * cps, trace), BF16),
            pltpu.VMEM((2 * cps, trace), F32),
            pltpu.VMEM((2 * cps, 2 * pair), F32),
            pltpu.VMEM((2, 2, 9 * cps, pair), BF16),
            pltpu.VMEM((2, 3 * cps, pair), BF16),
            pltpu.VMEM((cps, 5 * cps), F32),
            pltpu.VMEM((cps, 128), BF16),
            pltpu.VMEM((4, cps, 128), BF16),
            pltpu.VMEM((3, nz, nm, nc, cps // 2, 128), BF16),
            pltpu.VMEM((2, nz, 1, 128), F32),
            pltpu.VMEM((2, nm * nc, 1, 128), F32),
            pltpu.SemaphoreType.DMA((5,)),
            pltpu.SemaphoreType.DMA((copies,)),
            pltpu.SemaphoreType.DMA((copies,)),
        ],
        compiler_params=pltpu.CompilerParams(
            collective_id=0, has_side_effects=True, vmem_limit_bytes=50 * 1024 * 1024
        ),
    )(
        lead_side.reshape(2),
        keep(sources.reshape(2 * here, trace)),
        keep(impedance.reshape(2 * trace, trace)),
        keep(pair_maps.reshape(4, pair, pair)),
        keep(coarse_basis[0, 0]),
        keep(coarse_inverse),
    )
    return out.reshape(1, 1, 2, here, trace)


SHAPE = (8, 2, 4, 2, 2)


def build(mesh, shape):
    return jax.shard_map(
        functools.partial(per_device, shape),
        mesh=mesh,
        in_specs=(
            P("gx", "gy", None, "col", None),
            P("gx", "gy", None, None, None),
            P("gx", "gy", None, None, None, None),
            P("gx", "gy", None),
            P("gx", "gy", None, None, None),
            P(("gx", "gy", "col"), None),
        ),
        out_specs=P("gx", "gy", None, "col", None),
        check_vma=False,
    )


def solution(mesh):
    return build(mesh, SHAPE)
```

```python
import functools

import jax
import jax.numpy as jnp
from jax import lax
from jax.experimental import pallas as pl
from jax.experimental.pallas import tpu as pltpu
from jax.sharding import PartitionSpec as P

STEP_RATIO = 0.4
MESH = pl.DeviceIdType.MESH
F32 = jnp.float32
BF16 = jnp.bfloat16
HIGHEST = lax.Precision.HIGHEST


def dot(a, b, precision=None):
    return jnp.dot(a, b, preferred_element_type=F32, precision=precision)


def dot_nt(a, b, precision=None):
    return lax.dot_general(
        a, b, (((1,), (1,)), ((), ())), preferred_element_type=F32, precision=precision
    )


def dot_tn(a, b):
    return lax.dot_general(a, b, (((0,), (0,)), ((), ())), preferred_element_type=F32)


def split(x):
    high = x.astype(BF16)
    return high, (x - high.astype(F32)).astype(BF16)


def kernel(
    shape,
    lead_ref,
    src_hbm,
    imp_hbm,
    maps_hbm,
    basis_hbm,
    inv_hbm,
    out_ref,
    src,
    imp,
    maps,
    basis,
    inv,
    solver,
    inv_all,
    outgoing,
    image_out,
    face_out,
    face_in,
    image_in,
    ret_out,
    ret_in,
    solved_own,
    updated,
    state,
    rows,
    rows_turned,
    product,
    image,
    image_solved,
    proj_rows,
    basis_k,
    mapped,
    mapped_near,
    mapped_k,
    mapped_end,
    kernel_t,
    near_out,
    near_in,
    gathered,
    sum_z,
    sum_q,
    load_sem,
    send_sem,
    recv_sem,
):
    nz, nh, ny, nc, ncol = shape
    nm = nh * ny
    ngx, ngy = nz * nh, ny * nc
    sources = src.shape[0] // 2
    trace = src.shape[1]
    face = trace // 6
    pair = 2 * face
    cps = basis.shape[0]
    half = cps // 2

    gx, gy, col = lax.axis_index("gx"), lax.axis_index("gy"), lax.axis_index("col")
    z, xh = gx // nh, gx % nh
    y, core = gy // nc, gy % nc
    m = xh * ny + y

    def at(z_to, m_to, core_to):
        return {
            "gx": z_to * nh + m_to // ny,
            "gy": (m_to % ny) * nc + core_to,
            "col": col,
        }

    z_peers = [at((z + o) % nz, m, core) for o in range(1, nz)]
    m_peers = [at(z, (m + o) % nm, core) for o in range(1, nm)]
    c_peers = [at(z, m, (core + o) % nc) for o in range(1, nc)]
    q, nq = m * nc + core, nm * nc
    q_peers = [at(z, (q + o) % nq // nc, (q + o) % nq % nc) for o in range(1, nq)]
    offsets = [0]
    for o in range(1, nz // 2 + 1):
        offsets += [o] if 2 * o == nz else [o, nz - o]
    bounds = [0, 1] + list(range(3, nz - 2, 2)) + ([nz] if nz > 1 else [])
    groups = list(zip(bounds, bounds[1:]))
    below = [
        {"gx": (gx + ngx - 1) % ngx, "gy": gy, "col": col},
        {"gx": gx, "gy": (gy + ngy - 1) % ngy, "col": col},
    ]
    above = [
        {"gx": (gx + 1) % ngx, "gy": gy, "col": col},
        {"gx": gx, "gy": (gy + 1) % ngy, "col": col},
    ]
    col_peer = {"gx": gx, "gy": gy, "col": (col + 1) % ncol}
    position, last = [gx, gy], [ngx - 1, ngy - 1]

    loads = [
        pltpu.make_async_copy(a, b, load_sem.at[i])
        for i, (a, b) in enumerate(
            [(src_hbm, src), (maps_hbm, maps), (basis_hbm, basis), (inv_hbm, inv), (imp_hbm, imp)]
        )
    ]
    loads[0].start()

    barrier = pltpu.get_barrier_semaphore()
    partners = below + above + z_peers + q_peers + [col_peer]
    for partner in partners:
        pl.semaphore_signal(barrier, inc=1, device_id=partner, device_id_type=MESH)
    for i in (3, 1, 2, 4):
        loads[i].start()

    sent = []

    def remote(source, target, device):
        k = len(sent)
        copy = pltpu.make_async_remote_copy(
            src_ref=source,
            dst_ref=target,
            send_sem=send_sem.at[k],
            recv_sem=recv_sem.at[k],
            device_id=device,
            device_id_type=MESH,
        )
        copy.start()
        sent.append(copy)
        return copy

    def arrive(copies):
        for copy in copies:
            copy.wait_recv()

    def lanes(n):
        return lax.broadcasted_iota(jnp.int32, (n, 128), 1)

    def turned(x):
        part = x.shape[0] // 2
        return jnp.concatenate([-x[part:], x[:part]], axis=0)

    def packed_face(x):
        part = x.shape[0] // 2
        tail = jnp.where(
            lanes(part) < 64, x[:part, 128:256], pltpu.roll(x[part:, 128:256], 64, 1)
        )
        return jnp.concatenate([x[:, :128], tail], axis=0).astype(BF16)

    def face_parts(x):
        size = 2 * x.shape[0] // 3
        tail = x[size:].astype(F32)
        return x[:size].astype(F32), jnp.concatenate([tail, pltpu.roll(tail, 64, 1)], axis=0)

    def send_face(it, d):
        face_out[it, d] = packed_face(outgoing[it, :, pl.ds(d * pair, 256)].astype(F32))
        return remote(face_out.at[it, d], face_in.at[it, d], below[d])

    def solve(it, d, coming):
        coming[d].wait_recv()
        head, tail = face_parts(face_in[it, d])
        here = outgoing[it, :, pl.ds(d * pair, pair)]
        middle = jnp.where(lanes(2 * sources) < 64, tail, here[:, 128:256].astype(F32))
        x = jnp.concatenate([head.astype(BF16), middle.astype(BF16), here[:, 256:]], axis=1)
        solved = dot(x, solver[d, 0]) + dot(turned(x), solver[d, 1])
        ret_out[it, d] = packed_face(solved)
        solved_own[d] = solved[:, 128:]
        return remote(ret_out.at[it, d], ret_in.at[it, d], above[d])

    def assemble(it, returned):
        ends = outgoing[it, :, pl.ds(2 * pair, pair)].astype(F32)
        updated[it, :, pl.ds(2 * pair, pair)] = pltpu.roll(ends, face, 1)
        for d in range(2):
            returned[d].wait_recv()
            head, tail = face_parts(ret_in[it, d])
            own = jnp.where(position[d] < last[d], solved_own[d], 0.0)
            updated[it, :, pl.ds(d * pair, 128)] = jnp.where(position[d] > 0, head, 0.0)
            updated[it, :, pl.ds(d * pair + 128, 128)] = jnp.where(
                lanes(2 * sources) < 64, jnp.where(position[d] > 0, tail, 0.0), own[:, :128]
            )
            updated[it, :, pl.ds(d * pair + 256, 128)] = own[:, 128:]

    def apply_map(j):
        span = pl.ds(384 * j, 384)
        return dot(rows[...], imp[pl.ds(0, trace), span]) + dot(
            rows_turned[...], imp[pl.ds(trace, trace), span]
        )

    def packed(total):
        return jnp.where(
            lanes(half) < 64, total[:half], pltpu.roll(total[half:], sources, 1)
        ).astype(BF16)

    def project(defect):
        high, low = split(defect)
        first = dot_nt(proj_rows[...], high)
        second = dot_nt(proj_rows[pl.ds(0, 2 * cps), :], low)
        by_part = first[: 2 * cps] + first[2 * cps :] + second
        return packed(by_part[:cps] + pltpu.roll(by_part[cps:], sources, 1))

    def source_sums(products):
        folded = products[:, :128]
        for t in range(1, trace // 128):
            folded = folded + products[:, 128 * t : 128 * (t + 1)]
        folded = folded[:sources] + folded[sources:]
        both = jnp.concatenate([folded, folded], axis=0)
        return dot_nt(jnp.ones((8, 128), F32), both, HIGHEST)

    def forward(it, low, high):
        block = gathered.at[it, pl.ds(low, high - low), m, core]
        return [remote(block, block, peer) for peer in m_peers]

    def gather_start(it, block):
        gathered[it, 0, m, core] = block
        own = gathered.at[it, 0, m, core]
        coming = [None] * nz
        for i in range(nz - 1, 0, -1):
            coming[i] = remote(own, gathered.at[it, i, m, core], z_peers[offsets[i] - 1])
        return coming

    def gather_group(it, coming, low, high):
        arrive(coming[max(low, 1) : high])
        return forward(it, low, high)

    def gather_core(it, coming, low, high):
        arrive(coming)
        block = gathered.at[it, pl.ds(low, high - low), :, core]
        return [remote(block, block, peer) for peer in c_peers]

    def coarse_of(it, coming):
        arrive(coming)
        parts = 0.0
        for i in range(nz):
            parts = parts + dot(
                inv_all[i].reshape(2 * cps, nq * half), gathered[it, i].reshape(nq * half, 128)
            )
        return parts[:cps] + pltpu.roll(parts[cps:], sources, 1)

    def share(buffer, it, index, peers, row):
        buffer[it, index] = row[0:1]
        own = buffer.at[it, index]
        return [remote(own, own, peer) for peer in peers]

    def added(buffer, it, coming):
        arrive(coming)
        row = buffer[it, 0]
        for i in range(1, buffer.shape[1]):
            row = row + buffer[it, i]
        return jnp.broadcast_to(row, (8, 128))

    def stacked(coefficients):
        high, low = split(coefficients)
        return jnp.concatenate([high, low, high], axis=0)[:, :sources]

    def factor_of(total):
        return STEP_RATIO * jnp.sqrt(total / (pltpu.roll(total, sources, 1) + 1e-06))

    def energy_of(coarse):
        energy = jnp.sum(coarse * dot(gram, coarse, HIGHEST), axis=0, keepdims=True)
        return pltpu.roll(jnp.broadcast_to(energy, (8, 128)), sources, 1)

    def three(block):
        high, low = split(block)
        return jnp.concatenate([high, high, low], axis=0)

    def mapped_sum(near, c, d):
        if d == 2:
            return dot_tn(stacked(near[0]), mapped_end[c])
        coefficients = jnp.concatenate(
            [stacked(near[0]), stacked(near[1 + 2 * d]), stacked(near[2 + 2 * d])], axis=0
        )
        return dot_tn(coefficients, mapped_k[c, d])

    def against_basis(block, c, start, width):
        high, low = split(block)
        first = dot_nt(
            jnp.concatenate([high, low], axis=0),
            proj_rows[pl.ds(c * cps, cps), pl.ds(start, width)],
        )
        second = dot_nt(high, proj_rows[pl.ds((2 + c) * cps, cps), pl.ds(start, width)])
        return first[: block.shape[0]] + first[block.shape[0] :] + second

    def sides_of(c, d):
        part = mapped_near[pl.ds(c * cps, cps), pl.ds(d * pair, pair)]
        left = lax.broadcasted_iota(jnp.int32, (cps, pair), 1) < face
        return jnp.concatenate([jnp.where(left, part, 0.0), jnp.where(left, 0.0, part)], axis=0)

    loads[0].wait()
    outgoing[0] = src[...].astype(BF16)
    pl.semaphore_wait(barrier, len(partners))
    faces = [send_face(0, d) for d in range(2)]

    loads[2].wait()
    both = jnp.concatenate([basis[:, 0, :], basis[:, 1, :]], axis=0)
    high, low = split(both)
    proj_rows[pl.ds(0, 2 * cps), :] = high
    proj_rows[pl.ds(2 * cps, 2 * cps), :] = low
    for part, block in enumerate((high, low)):
        rows[pl.ds(part * 2 * cps, 2 * cps), :] = block
        rows_turned[pl.ds(part * 2 * cps, 2 * cps), :] = turned(block)

    loads[4].wait()

    def apply_to_basis(j):
        whole = apply_map(j)
        whole = whole[: 2 * cps] + whole[2 * cps :]
        image[:, pl.ds(384 * j, 384)] = whole
        return whole

    image_coming = []

    def send_image(j):
        image_out[j] = packed_face(apply_to_basis(j))
        image_coming.append(remote(image_out.at[j], image_in.at[j], below[j]))

    send_image(0)
    loads[1].wait()
    for d in range(2):
        for c in range(2):
            stored = maps[2 * d + c].astype(F32)
            swapped = jnp.concatenate([stored[face:], stored[:face]], axis=0)
            swapped = pltpu.roll(swapped, face, 1)
            solver[d, c] = jnp.where(lead_ref[d] == 0, swapped, stored).astype(BF16)
    returned = [solve(0, 0, faces)]
    send_image(1)
    returned.append(solve(0, 1, faces))
    apply_to_basis(2)

    loads[3].wait()
    here = lax.broadcasted_iota(jnp.int32, (256, 256), 0)
    there = lax.broadcasted_iota(jnp.int32, (256, 256), 1)
    wanted = ((here // half) % 2) * 128 + (here // cps) * half + here % half
    order = jnp.where(there == wanted, 1.0, 0.0).astype(BF16)
    chunks = nq * cps // 256
    for i in range(nz):
        source_z = (z + nz - offsets[i]) % nz
        for j in range(chunks):
            start = pl.multiple_of((source_z * chunks + j) * 256, 256)
            moved = dot(inv[:, pl.ds(start, 256)].astype(BF16), order).astype(BF16)
            for h in range(2):
                inv_all[i, h, col, :, pl.ds(128 * j, 128)] = moved[:, 128 * h : 128 * (h + 1)]

    image_returned = []
    for d in range(2):
        image_coming[d].wait_recv()
        head, tail = face_parts(image_in[d])
        own = image[:, pl.ds(d * pair, pair)]
        low_lane = lanes(2 * cps) < 64
        zero = jnp.zeros((2 * cps, 128), F32)
        x = jnp.concatenate(
            [zero, jnp.where(low_lane, 0.0, own[:, 128:256]), own[:, 256:]], axis=1
        ).astype(BF16)
        w = jnp.concatenate(
            [head, jnp.where(low_lane, tail, 0.0), zero], axis=1
        ).astype(BF16)
        solved = dot(jnp.concatenate([x, w], axis=0), solver[d, 0]) + dot(
            jnp.concatenate([turned(x), turned(w)], axis=0), solver[d, 1]
        )
        ret_out[2, d] = packed_face(solved)
        image_solved[d] = solved[:, 128:]
        image_returned.append(remote(ret_out.at[2, d], ret_in.at[2, d], above[d]))
    gram = dot_nt(both[:cps], both[:cps], HIGHEST) + dot_nt(both[cps:], both[cps:], HIGHEST)
    for c in range(2):
        basis_k[c] = three(both[c * cps : (c + 1) * cps])
    assemble(0, returned)

    coming = gather_start(0, project(updated[0]))
    inverse_coming = remote(inv_all.at[:, :, col], inv_all.at[:, :, col], col_peer)
    moving = [gather_group(0, coming, *groups[0])]
    high = updated[0].astype(BF16)
    rows[...] = high
    rows_turned[...] = turned(high)
    faces_next = []
    for j in range(trace // 384):
        if j == 2:
            for group in groups[3:]:
                moving.append(gather_group(0, coming, *group))
        span = pl.ds(384 * j, 384)
        outgoing[1, :, span] = (apply_map(j) + src[:, span]).astype(BF16)
        if j < 2:
            faces_next.append(send_face(1, j))
            if j + 1 < len(groups):
                moving.append(gather_group(0, coming, *groups[j + 1]))

    first_squares = source_sums(updated[0] * updated[0])
    split_at = groups[-1][0]
    returned = [solve(1, d, faces_next) for d in range(2)]
    coming = gather_core(0, sum(moving[:-1], []), 0, split_at)
    coming += gather_core(0, moving[-1], split_at, nz)

    inverse_coming.wait_recv()
    coarse = coarse_of(0, coming)
    high, low = split(coarse)
    near_out[...] = jnp.where(
        lanes(cps) < 64, high.astype(F32), pltpu.roll(low.astype(F32), sources, 1)
    ).astype(BF16)
    near_coming = []
    for d in range(2):
        near_coming.append(remote(near_out, near_in.at[2 * d], above[d]))
        near_coming.append(remote(near_out, near_in.at[2 * d + 1], below[d]))
    first_row = jnp.where(lanes(8) < 64, first_squares, energy_of(coarse))
    for d in range(2):
        image_returned[d].wait_recv()
        back = jnp.concatenate(face_parts(ret_in[2, d]), axis=1)
        back = jnp.where(position[d] > 0, back, 0.0)
        own = jnp.where(position[d] < last[d], image_solved[d], 0.0)
        for target, r, o in ((mapped, 2 * cps, 0), (mapped_near, 0, 2 * cps)):
            target[:, pl.ds(d * pair, 128)] = back[r : r + 2 * cps, :128]
            target[:, pl.ds(d * pair + 128, 128)] = jnp.where(
                lanes(2 * cps) < 64, back[r : r + 2 * cps, 128:], own[o : o + 2 * cps, :128]
            )
            target[:, pl.ds(d * pair + 256, 128)] = own[o : o + 2 * cps, 128:]
    mapped[:, pl.ds(2 * pair, pair)] = pltpu.roll(image[:, pl.ds(2 * pair, pair)], face, 1)
    moved = mapped[...] - both
    blocks = [
        against_basis(moved[:cps], 0, 0, trace) + against_basis(moved[cps:], 1, 0, trace)
    ]
    for d in range(2):
        blocks.append(
            against_basis(sides_of(0, d), 0, d * pair, pair)
            + against_basis(sides_of(1, d), 1, d * pair, pair)
        )
    kernel_t[...] = jnp.concatenate(blocks, axis=0).T


    assemble(1, returned)
    state[...] = updated[1] - updated[0]
    early = gather_start(2, project(state[...]))

    arrive(near_coming)
    near = [coarse]
    for i in range(4):
        both_parts = near_in[i].astype(F32)
        near.append(both_parts + pltpu.roll(both_parts, sources, 1))
    coming = gather_start(
        1, packed(dot(kernel_t[...], jnp.concatenate(near, axis=0), HIGHEST))
    )
    norms = share(sum_z, 0, z, z_peers, first_row)
    moving = [gather_group(1, coming, *groups[0])]
    for c in range(2):
        for d in range(2):
            sides = sides_of(c, d)
            own = three(mapped[pl.ds(c * cps, cps), pl.ds(d * pair, pair)])
            mapped_k[c, d] = jnp.concatenate(
                [own, three(sides[:cps]), three(sides[cps:])], axis=0
            )
        mapped_end[c] = three(mapped[pl.ds(c * cps, cps), pl.ds(2 * pair, pair)])
    early = gather_group(2, early, 0, nz)
    for c in range(2):
        part = pl.ds(c * sources, sources)
        for d in range(3):
            product[part, pl.ds(d * pair, pair)] = mapped_sum(near, c, d)
        product[part, :] = product[part, :] - dot_tn(stacked(coarse), basis_k[c])
        if c + 1 < len(groups):
            moving.append(gather_group(1, coming, *groups[c + 1]))
    for group in groups[3:]:
        moving.append(gather_group(1, coming, *group))
    norms = share(sum_q, 0, q, q_peers, added(sum_z, 0, norms))
    sums_aa = source_sums(state[...] * state[...])
    sums_ab = source_sums(state[...] * product[...])
    sums_bb = source_sums(product[...] * product[...])
    early = gather_core(2, early, 0, nz)
    late = gather_core(1, sum(moving[:-1], []), 0, split_at)
    coarse_early = coarse_of(2, early)
    late += gather_core(1, moving[-1], split_at, nz)
    factor = factor_of(added(sum_q, 0, norms))
    coarse = coarse_early + factor[0:1] * coarse_of(1, late)
    squares = sums_aa + factor * (2.0 * sums_ab + factor * sums_bb)
    row = jnp.where(lanes(8) < 64, squares, energy_of(coarse))
    norms = share(sum_z, 1, z, z_peers, row)
    near = [factor[0:1] * part for part in near]
    for c in range(2):
        part = pl.ds(c * sources, sources)
        for d in range(3):
            span = pl.ds(d * pair, pair)
            updated[1, part, span] = updated[1, part, span] + mapped_sum(near, c, d)
    norms = share(sum_q, 1, q, q_peers, added(sum_z, 1, norms))
    factor = factor_of(added(sum_q, 1, norms))
    scaled = stacked(factor[0:1] * coarse)
    for c in range(2):
        part = pl.ds(c * sources, sources)
        out_ref[part, :] = updated[1, part, :] + dot_tn(scaled, basis_k[c])
    for copy in sent:
        copy.wait_send()


def per_device(shape, sources, impedance, pair_maps, lead_side, coarse_basis, coarse_inverse):
    nz, nh, ny, nc, ncol = shape
    here, trace = sources.shape[3], sources.shape[4]
    pair = pair_maps.shape[-1]
    cps = coarse_basis.shape[2]
    size = coarse_inverse.shape[1]
    nm = nh * ny
    copies = 1 + 3 * 4 + 4 + 3 * (nz - 1) + 9 * (nm - 1) + 5 * (nc - 1)
    copies += 2 * (nz - 1 + nm * nc - 1)
    def keep(array):
        return pltpu.with_memory_space_constraint(array, pltpu.HBM)

    hbm = pl.BlockSpec(memory_space=pltpu.HBM)
    out = pl.pallas_call(
        functools.partial(kernel, shape),
        out_shape=jax.ShapeDtypeStruct((2 * here, trace), F32),
        in_specs=[pl.BlockSpec(memory_space=pltpu.SMEM)] + [hbm] * 5,
        out_specs=pl.BlockSpec(memory_space=pltpu.VMEM),
        scratch_shapes=[
            pltpu.VMEM((2 * here, trace), F32),
            pltpu.VMEM((2 * trace, trace), BF16),
            pltpu.VMEM((4, pair, pair), BF16),
            pltpu.VMEM((cps, 2, trace), F32),
            pltpu.VMEM((cps // 2, size), F32),
            pltpu.VMEM((2, 2, pair, pair), BF16),
            pltpu.VMEM((nz, 2, ncol, cps // 2, nm * nc * cps // 2), BF16),
            pltpu.VMEM((2, 2 * here, trace), BF16),
            pltpu.VMEM((2, 3 * cps, 128), BF16),
            pltpu.VMEM((2, 2, 3 * here, 128), BF16),
            pltpu.VMEM((2, 2, 3 * here, 128), BF16),
            pltpu.VMEM((2, 3 * cps, 128), BF16),
            pltpu.VMEM((3, 2, 3 * here, 128), BF16),
            pltpu.VMEM((3, 2, 3 * here, 128), BF16),
            pltpu.VMEM((2, 2 * here, 256), F32),
            pltpu.VMEM((2, 2 * here, trace), F32),
            pltpu.VMEM((2 * here, trace), F32),
            pltpu.VMEM((2 * here, trace), BF16),
            pltpu.VMEM((2 * here, trace), BF16),
            pltpu.VMEM((2 * here, trace), F32),
            pltpu.VMEM((2 * cps, trace), F32),
            pltpu.VMEM((2, 4 * cps, 256), F32),
            pltpu.VMEM((4 * cps, trace), BF16),
            pltpu.VMEM((2, 3 * cps, trace), BF16),
            pltpu.VMEM((2 * cps, trace), F32),
            pltpu.VMEM((2 * cps, 2 * pair), F32),
            pltpu.VMEM((2, 2, 9 * cps, pair), BF16),
            pltpu.VMEM((2, 3 * cps, pair), BF16),
            pltpu.VMEM((cps, 5 * cps), F32),
            pltpu.VMEM((cps, 128), BF16),
            pltpu.VMEM((4, cps, 128), BF16),
            pltpu.VMEM((3, nz, nm, nc, cps // 2, 128), BF16),
            pltpu.VMEM((2, nz, 1, 128), F32),
            pltpu.VMEM((2, nm * nc, 1, 128), F32),
            pltpu.SemaphoreType.DMA((5,)),
            pltpu.SemaphoreType.DMA((copies,)),
            pltpu.SemaphoreType.DMA((copies,)),
        ],
        compiler_params=pltpu.CompilerParams(
            collective_id=0, has_side_effects=True, vmem_limit_bytes=50 * 1024 * 1024
        ),
    )(
        lead_side.reshape(2),
        keep(sources.reshape(2 * here, trace)),
        keep(impedance.reshape(2 * trace, trace)),
        keep(pair_maps.reshape(4, pair, pair)),
        keep(coarse_basis[0, 0]),
        keep(coarse_inverse),
    )
    return out.reshape(1, 1, 2, here, trace)


SHAPE = (8, 2, 4, 2, 2)


def build(mesh, shape):
    return jax.shard_map(
        functools.partial(per_device, shape),
        mesh=mesh,
        in_specs=(
            P("gx", "gy", None, "col", None),
            P("gx", "gy", None, None, None),
            P("gx", "gy", None, None, None, None),
            P("gx", "gy", None),
            P("gx", "gy", None, None, None),
            P(("gx", "gy", "col"), None),
        ),
        out_specs=P("gx", "gy", None, "col", None),
        check_vma=False,
    )


def solution(mesh):
    return build(mesh, SHAPE)
```

```python
import functools

import jax
import jax.numpy as jnp
from jax import lax
from jax.experimental import pallas as pl
from jax.experimental.pallas import tpu as pltpu
from jax.sharding import PartitionSpec as P

STEP_RATIO = 0.4
MESH = pl.DeviceIdType.MESH
F32 = jnp.float32
BF16 = jnp.bfloat16
HIGHEST = lax.Precision.HIGHEST


def dot(a, b, precision=None):
    return jnp.dot(a, b, preferred_element_type=F32, precision=precision)


def dot_nt(a, b, precision=None):
    return lax.dot_general(
        a, b, (((1,), (1,)), ((), ())), preferred_element_type=F32, precision=precision
    )


def dot_tn(a, b):
    return lax.dot_general(a, b, (((0,), (0,)), ((), ())), preferred_element_type=F32)


def split(x):
    high = x.astype(BF16)
    return high, (x - high.astype(F32)).astype(BF16)


def kernel(
    shape,
    lead_ref,
    src_hbm,
    imp_hbm,
    maps_hbm,
    basis_hbm,
    inv_hbm,
    out_ref,
    src,
    imp,
    maps,
    basis,
    inv,
    solver,
    inv_all,
    outgoing,
    image_out,
    face_out,
    face_in,
    image_in,
    ret_out,
    ret_in,
    solved_own,
    updated,
    state,
    rows,
    rows_turned,
    product,
    image,
    image_solved,
    proj_rows,
    basis_k,
    mapped,
    mapped_near,
    mapped_k,
    mapped_end,
    kernel_t,
    near_out,
    near_in,
    gathered,
    sum_z,
    sum_q,
    load_sem,
    send_sem,
    recv_sem,
):
    nz, nh, ny, nc, ncol = shape
    nm = nh * ny
    ngx, ngy = nz * nh, ny * nc
    sources = src.shape[0] // 2
    trace = src.shape[1]
    face = trace // 6
    pair = 2 * face
    cps = basis.shape[0]
    half = cps // 2

    gx, gy, col = lax.axis_index("gx"), lax.axis_index("gy"), lax.axis_index("col")
    z, xh = gx // nh, gx % nh
    y, core = gy // nc, gy % nc
    m = xh * ny + y

    def at(z_to, m_to, core_to):
        return {
            "gx": z_to * nh + m_to // ny,
            "gy": (m_to % ny) * nc + core_to,
            "col": col,
        }

    z_peers = [at((z + o) % nz, m, core) for o in range(1, nz)]
    m_peers = [at(z, (m + o) % nm, core) for o in range(1, nm)]
    c_peers = [at(z, m, (core + o) % nc) for o in range(1, nc)]
    q, nq = m * nc + core, nm * nc
    q_peers = [at(z, (q + o) % nq // nc, (q + o) % nq % nc) for o in range(1, nq)]
    offsets = [0]
    for o in range(1, nz // 2 + 1):
        offsets += [o] if 2 * o == nz else [o, nz - o]
    bounds = [0, 1] + list(range(3, nz - 2, 2)) + ([nz] if nz > 1 else [])
    groups = list(zip(bounds, bounds[1:]))
    below = [
        {"gx": (gx + ngx - 1) % ngx, "gy": gy, "col": col},
        {"gx": gx, "gy": (gy + ngy - 1) % ngy, "col": col},
    ]
    above = [
        {"gx": (gx + 1) % ngx, "gy": gy, "col": col},
        {"gx": gx, "gy": (gy + 1) % ngy, "col": col},
    ]
    col_peer = {"gx": gx, "gy": gy, "col": (col + 1) % ncol}
    position, last = [gx, gy], [ngx - 1, ngy - 1]

    loads = [
        pltpu.make_async_copy(a, b, load_sem.at[i])
        for i, (a, b) in enumerate(
            [(src_hbm, src), (maps_hbm, maps), (basis_hbm, basis), (inv_hbm, inv), (imp_hbm, imp)]
        )
    ]
    loads[0].start()

    barrier = pltpu.get_barrier_semaphore()
    partners = below + above + z_peers + q_peers + [col_peer]
    for partner in partners:
        pl.semaphore_signal(barrier, inc=1, device_id=partner, device_id_type=MESH)
    for i in (3, 1, 2, 4):
        loads[i].start()

    sent = []

    def remote(source, target, device):
        k = len(sent)
        copy = pltpu.make_async_remote_copy(
            src_ref=source,
            dst_ref=target,
            send_sem=send_sem.at[k],
            recv_sem=recv_sem.at[k],
            device_id=device,
            device_id_type=MESH,
        )
        copy.start()
        sent.append(copy)
        return copy

    def arrive(copies):
        for copy in copies:
            copy.wait_recv()

    def lanes(n):
        return lax.broadcasted_iota(jnp.int32, (n, 128), 1)

    def turned(x):
        part = x.shape[0] // 2
        return jnp.concatenate([-x[part:], x[:part]], axis=0)

    def packed_face(x):
        part = x.shape[0] // 2
        tail = jnp.where(
            lanes(part) < 64, x[:part, 128:256], pltpu.roll(x[part:, 128:256], 64, 1)
        )
        return jnp.concatenate([x[:, :128], tail], axis=0).astype(BF16)

    def face_parts(x):
        size = 2 * x.shape[0] // 3
        tail = x[size:].astype(F32)
        return x[:size].astype(F32), jnp.concatenate([tail, pltpu.roll(tail, 64, 1)], axis=0)

    def send_face(it, d):
        face_out[it, d] = packed_face(outgoing[it, :, pl.ds(d * pair, 256)].astype(F32))
        return remote(face_out.at[it, d], face_in.at[it, d], below[d])

    def solve(it, d, coming):
        coming[d].wait_recv()
        head, tail = face_parts(face_in[it, d])
        here = outgoing[it, :, pl.ds(d * pair, pair)]
        middle = jnp.where(lanes(2 * sources) < 64, tail, here[:, 128:256].astype(F32))
        x = jnp.concatenate([head.astype(BF16), middle.astype(BF16), here[:, 256:]], axis=1)
        solved = dot(x, solver[d, 0]) + dot(turned(x), solver[d, 1])
        ret_out[it, d] = packed_face(solved)
        solved_own[d] = solved[:, 128:]
        return remote(ret_out.at[it, d], ret_in.at[it, d], above[d])

    def assemble(it, returned):
        ends = outgoing[it, :, pl.ds(2 * pair, pair)].astype(F32)
        updated[it, :, pl.ds(2 * pair, pair)] = pltpu.roll(ends, face, 1)
        for d in range(2):
            returned[d].wait_recv()
            head, tail = face_parts(ret_in[it, d])
            own = jnp.where(position[d] < last[d], solved_own[d], 0.0)
            updated[it, :, pl.ds(d * pair, 128)] = jnp.where(position[d] > 0, head, 0.0)
            updated[it, :, pl.ds(d * pair + 128, 128)] = jnp.where(
                lanes(2 * sources) < 64, jnp.where(position[d] > 0, tail, 0.0), own[:, :128]
            )
            updated[it, :, pl.ds(d * pair + 256, 128)] = own[:, 128:]

    def apply_map(j):
        span = pl.ds(384 * j, 384)
        return dot(rows[...], imp[pl.ds(0, trace), span]) + dot(
            rows_turned[...], imp[pl.ds(trace, trace), span]
        )

    def packed(total):
        return jnp.where(
            lanes(half) < 64, total[:half], pltpu.roll(total[half:], sources, 1)
        ).astype(BF16)

    def project(defect):
        high, low = split(defect)
        first = dot_nt(proj_rows[...], high)
        second = dot_nt(proj_rows[pl.ds(0, 2 * cps), :], low)
        by_part = first[: 2 * cps] + first[2 * cps :] + second
        return packed(by_part[:cps] + pltpu.roll(by_part[cps:], sources, 1))

    def source_sums(products):
        folded = products[:, :128]
        for t in range(1, trace // 128):
            folded = folded + products[:, 128 * t : 128 * (t + 1)]
        folded = folded[:sources] + folded[sources:]
        both = jnp.concatenate([folded, folded], axis=0)
        return dot_nt(jnp.ones((8, 128), F32), both, HIGHEST)

    def forward(it, low, high):
        block = gathered.at[it, pl.ds(low, high - low), m, core]
        return [remote(block, block, peer) for peer in m_peers]

    def gather_start(it, block):
        gathered[it, 0, m, core] = block
        own = gathered.at[it, 0, m, core]
        coming = [None] * nz
        for i in range(nz - 1, 0, -1):
            coming[i] = remote(own, gathered.at[it, i, m, core], z_peers[offsets[i] - 1])
        return coming

    def gather_group(it, coming, low, high):
        arrive(coming[max(low, 1) : high])
        return forward(it, low, high)

    def gather_core(it, coming, low, high):
        arrive(coming)
        block = gathered.at[it, pl.ds(low, high - low), :, core]
        return [remote(block, block, peer) for peer in c_peers]

    def coarse_of(it, coming):
        arrive(coming)
        parts = 0.0
        for i in range(nz):
            parts = parts + dot(
                inv_all[i].reshape(2 * cps, nq * half), gathered[it, i].reshape(nq * half, 128)
            )
        return parts[:cps] + pltpu.roll(parts[cps:], sources, 1)

    def share(buffer, it, index, peers, row):
        buffer[it, index] = row[0:1]
        own = buffer.at[it, index]
        return [remote(own, own, peer) for peer in peers]

    def added(buffer, it, coming):
        arrive(coming)
        row = buffer[it, 0]
        for i in range(1, buffer.shape[1]):
            row = row + buffer[it, i]
        return jnp.broadcast_to(row, (8, 128))

    def stacked(coefficients):
        high, low = split(coefficients)
        return jnp.concatenate([high, low, high], axis=0)[:, :sources]

    def factor_of(total):
        return STEP_RATIO * jnp.sqrt(total / (pltpu.roll(total, sources, 1) + 1e-06))

    def energy_of(coarse):
        energy = jnp.sum(coarse * dot(gram, coarse, HIGHEST), axis=0, keepdims=True)
        return pltpu.roll(jnp.broadcast_to(energy, (8, 128)), sources, 1)

    def three(block):
        high, low = split(block)
        return jnp.concatenate([high, high, low], axis=0)

    def mapped_sum(near, c, d):
        if d == 2:
            return dot_tn(stacked(near[0]), mapped_end[c])
        coefficients = jnp.concatenate(
            [stacked(near[0]), stacked(near[1 + 2 * d]), stacked(near[2 + 2 * d])], axis=0
        )
        return dot_tn(coefficients, mapped_k[c, d])

    def against_basis(block, c, start, width):
        high, low = split(block)
        first = dot_nt(
            jnp.concatenate([high, low], axis=0),
            proj_rows[pl.ds(c * cps, cps), pl.ds(start, width)],
        )
        second = dot_nt(high, proj_rows[pl.ds((2 + c) * cps, cps), pl.ds(start, width)])
        return first[: block.shape[0]] + first[block.shape[0] :] + second

    def sides_of(c, d):
        part = mapped_near[pl.ds(c * cps, cps), pl.ds(d * pair, pair)]
        left = lax.broadcasted_iota(jnp.int32, (cps, pair), 1) < face
        return jnp.concatenate([jnp.where(left, part, 0.0), jnp.where(left, 0.0, part)], axis=0)

    loads[0].wait()
    outgoing[0] = src[...].astype(BF16)
    pl.semaphore_wait(barrier, len(partners))
    faces = [send_face(0, d) for d in range(2)]

    loads[2].wait()
    both = jnp.concatenate([basis[:, 0, :], basis[:, 1, :]], axis=0)
    high, low = split(both)
    proj_rows[pl.ds(0, 2 * cps), :] = high
    proj_rows[pl.ds(2 * cps, 2 * cps), :] = low
    for part, block in enumerate((high, low)):
        rows[pl.ds(part * 2 * cps, 2 * cps), :] = block
        rows_turned[pl.ds(part * 2 * cps, 2 * cps), :] = turned(block)

    loads[4].wait()

    def apply_to_basis(j):
        whole = apply_map(j)
        whole = whole[: 2 * cps] + whole[2 * cps :]
        image[:, pl.ds(384 * j, 384)] = whole
        return whole

    image_coming = []

    def send_image(j):
        image_out[j] = packed_face(apply_to_basis(j))
        image_coming.append(remote(image_out.at[j], image_in.at[j], below[j]))

    send_image(0)
    loads[1].wait()
    for d in range(2):
        for c in range(2):
            stored = maps[2 * d + c].astype(F32)
            swapped = jnp.concatenate([stored[face:], stored[:face]], axis=0)
            swapped = pltpu.roll(swapped, face, 1)
            solver[d, c] = jnp.where(lead_ref[d] == 0, swapped, stored).astype(BF16)
    returned = [solve(0, 0, faces)]
    send_image(1)
    returned.append(solve(0, 1, faces))
    apply_to_basis(2)

    loads[3].wait()
    here = lax.broadcasted_iota(jnp.int32, (256, 256), 0)
    there = lax.broadcasted_iota(jnp.int32, (256, 256), 1)
    wanted = ((here // half) % 2) * 128 + (here // cps) * half + here % half
    order = jnp.where(there == wanted, 1.0, 0.0).astype(BF16)
    chunks = nq * cps // 256
    for i in range(nz):
        source_z = (z + nz - offsets[i]) % nz
        for j in range(chunks):
            start = pl.multiple_of((source_z * chunks + j) * 256, 256)
            moved = dot(inv[:, pl.ds(start, 256)].astype(BF16), order).astype(BF16)
            for h in range(2):
                inv_all[i, h, col, :, pl.ds(128 * j, 128)] = moved[:, 128 * h : 128 * (h + 1)]

    image_returned = []
    for d in range(2):
        image_coming[d].wait_recv()
        head, tail = face_parts(image_in[d])
        own = image[:, pl.ds(d * pair, pair)]
        low_lane = lanes(2 * cps) < 64
        zero = jnp.zeros((2 * cps, 128), F32)
        x = jnp.concatenate(
            [zero, jnp.where(low_lane, 0.0, own[:, 128:256]), own[:, 256:]], axis=1
        ).astype(BF16)
        w = jnp.concatenate(
            [head, jnp.where(low_lane, tail, 0.0), zero], axis=1
        ).astype(BF16)
        solved = dot(jnp.concatenate([x, w], axis=0), solver[d, 0]) + dot(
            jnp.concatenate([turned(x), turned(w)], axis=0), solver[d, 1]
        )
        ret_out[2, d] = packed_face(solved)
        image_solved[d] = solved[:, 128:]
        image_returned.append(remote(ret_out.at[2, d], ret_in.at[2, d], above[d]))
    assemble(0, returned)

    coming = gather_start(0, project(updated[0]))
    inverse_coming = remote(inv_all.at[:, :, col], inv_all.at[:, :, col], col_peer)
    moving = [gather_group(0, coming, *groups[0])]
    high = updated[0].astype(BF16)
    rows[...] = high
    rows_turned[...] = turned(high)
    faces_next = []
    for j in range(trace // 384):
        if j == 2:
            for group in groups[3:]:
                moving.append(gather_group(0, coming, *group))
        span = pl.ds(384 * j, 384)
        outgoing[1, :, span] = (apply_map(j) + src[:, span]).astype(BF16)
        if j < 2:
            faces_next.append(send_face(1, j))
            if j + 1 < len(groups):
                moving.append(gather_group(0, coming, *groups[j + 1]))

    first_squares = source_sums(updated[0] * updated[0])
    gram = dot_nt(both[:cps], both[:cps], HIGHEST) + dot_nt(both[cps:], both[cps:], HIGHEST)
    for c in range(2):
        basis_k[c] = three(both[c * cps : (c + 1) * cps])
    split_at = groups[-1][0]
    returned = [solve(1, d, faces_next) for d in range(2)]
    coming = gather_core(0, sum(moving[:-1], []), 0, split_at)
    coming += gather_core(0, moving[-1], split_at, nz)

    inverse_coming.wait_recv()
    coarse = coarse_of(0, coming)
    high, low = split(coarse)
    near_out[...] = jnp.where(
        lanes(cps) < 64, high.astype(F32), pltpu.roll(low.astype(F32), sources, 1)
    ).astype(BF16)
    near_coming = []
    for d in range(2):
        near_coming.append(remote(near_out, near_in.at[2 * d], above[d]))
        near_coming.append(remote(near_out, near_in.at[2 * d + 1], below[d]))
    first_row = jnp.where(lanes(8) < 64, first_squares, energy_of(coarse))
    for d in range(2):
        image_returned[d].wait_recv()
        back = jnp.concatenate(face_parts(ret_in[2, d]), axis=1)
        back = jnp.where(position[d] > 0, back, 0.0)
        own = jnp.where(position[d] < last[d], image_solved[d], 0.0)
        for target, r, o in ((mapped, 2 * cps, 0), (mapped_near, 0, 2 * cps)):
            target[:, pl.ds(d * pair, 128)] = back[r : r + 2 * cps, :128]
            target[:, pl.ds(d * pair + 128, 128)] = jnp.where(
                lanes(2 * cps) < 64, back[r : r + 2 * cps, 128:], own[o : o + 2 * cps, :128]
            )
            target[:, pl.ds(d * pair + 256, 128)] = own[o : o + 2 * cps, 128:]
    mapped[:, pl.ds(2 * pair, pair)] = pltpu.roll(image[:, pl.ds(2 * pair, pair)], face, 1)
    moved = mapped[...] - both
    blocks = [
        against_basis(moved[:cps], 0, 0, trace) + against_basis(moved[cps:], 1, 0, trace)
    ]
    for d in range(2):
        blocks.append(
            against_basis(sides_of(0, d), 0, d * pair, pair)
            + against_basis(sides_of(1, d), 1, d * pair, pair)
        )
    kernel_t[...] = jnp.concatenate(blocks, axis=0).T


    assemble(1, returned)
    state[...] = updated[1] - updated[0]
    early = gather_start(2, project(state[...]))

    arrive(near_coming)
    near = [coarse]
    for i in range(4):
        both_parts = near_in[i].astype(F32)
        near.append(both_parts + pltpu.roll(both_parts, sources, 1))
    coming = gather_start(
        1, packed(dot(kernel_t[...], jnp.concatenate(near, axis=0), HIGHEST))
    )
    norms = share(sum_z, 0, z, z_peers, first_row)
    moving = [gather_group(1, coming, *groups[0])]
    for c in range(2):
        for d in range(2):
            sides = sides_of(c, d)
            own = three(mapped[pl.ds(c * cps, cps), pl.ds(d * pair, pair)])
            mapped_k[c, d] = jnp.concatenate(
                [own, three(sides[:cps]), three(sides[cps:])], axis=0
            )
        mapped_end[c] = three(mapped[pl.ds(c * cps, cps), pl.ds(2 * pair, pair)])
    early = gather_group(2, early, 0, nz)
    for c in range(2):
        part = pl.ds(c * sources, sources)
        for d in range(3):
            product[part, pl.ds(d * pair, pair)] = mapped_sum(near, c, d)
        product[part, :] = product[part, :] - dot_tn(stacked(coarse), basis_k[c])
        if c + 1 < len(groups):
            moving.append(gather_group(1, coming, *groups[c + 1]))
    for group in groups[3:]:
        moving.append(gather_group(1, coming, *group))
    norms = share(sum_q, 0, q, q_peers, added(sum_z, 0, norms))
    sums_aa = source_sums(state[...] * state[...])
    sums_ab = source_sums(state[...] * product[...])
    sums_bb = source_sums(product[...] * product[...])
    early = gather_core(2, early, 0, nz)
    late = gather_core(1, sum(moving[:-1], []), 0, split_at)
    coarse_early = coarse_of(2, early)
    late += gather_core(1, moving[-1], split_at, nz)
    factor = factor_of(added(sum_q, 0, norms))
    coarse = coarse_early + factor[0:1] * coarse_of(1, late)
    squares = sums_aa + factor * (2.0 * sums_ab + factor * sums_bb)
    row = jnp.where(lanes(8) < 64, squares, energy_of(coarse))
    norms = share(sum_z, 1, z, z_peers, row)
    near = [factor[0:1] * part for part in near]
    for c in range(2):
        part = pl.ds(c * sources, sources)
        for d in range(3):
            span = pl.ds(d * pair, pair)
            updated[1, part, span] = updated[1, part, span] + mapped_sum(near, c, d)
    norms = share(sum_q, 1, q, q_peers, added(sum_z, 1, norms))
    factor = factor_of(added(sum_q, 1, norms))
    scaled = stacked(factor[0:1] * coarse)
    for c in range(2):
        part = pl.ds(c * sources, sources)
        out_ref[part, :] = updated[1, part, :] + dot_tn(scaled, basis_k[c])
    for copy in sent:
        copy.wait_send()


def per_device(shape, sources, impedance, pair_maps, lead_side, coarse_basis, coarse_inverse):
    nz, nh, ny, nc, ncol = shape
    here, trace = sources.shape[3], sources.shape[4]
    pair = pair_maps.shape[-1]
    cps = coarse_basis.shape[2]
    size = coarse_inverse.shape[1]
    nm = nh * ny
    copies = 1 + 3 * 4 + 4 + 3 * (nz - 1) + 9 * (nm - 1) + 5 * (nc - 1)
    copies += 2 * (nz - 1 + nm * nc - 1)
    def keep(array):
        return pltpu.with_memory_space_constraint(array, pltpu.HBM)

    hbm = pl.BlockSpec(memory_space=pltpu.HBM)
    out = pl.pallas_call(
        functools.partial(kernel, shape),
        out_shape=jax.ShapeDtypeStruct((2 * here, trace), F32),
        in_specs=[pl.BlockSpec(memory_space=pltpu.SMEM)] + [hbm] * 5,
        out_specs=pl.BlockSpec(memory_space=pltpu.VMEM),
        scratch_shapes=[
            pltpu.VMEM((2 * here, trace), F32),
            pltpu.VMEM((2 * trace, trace), BF16),
            pltpu.VMEM((4, pair, pair), BF16),
            pltpu.VMEM((cps, 2, trace), F32),
            pltpu.VMEM((cps // 2, size), F32),
            pltpu.VMEM((2, 2, pair, pair), BF16),
            pltpu.VMEM((nz, 2, ncol, cps // 2, nm * nc * cps // 2), BF16),
            pltpu.VMEM((2, 2 * here, trace), BF16),
            pltpu.VMEM((2, 3 * cps, 128), BF16),
            pltpu.VMEM((2, 2, 3 * here, 128), BF16),
            pltpu.VMEM((2, 2, 3 * here, 128), BF16),
            pltpu.VMEM((2, 3 * cps, 128), BF16),
            pltpu.VMEM((3, 2, 3 * here, 128), BF16),
            pltpu.VMEM((3, 2, 3 * here, 128), BF16),
            pltpu.VMEM((2, 2 * here, 256), F32),
            pltpu.VMEM((2, 2 * here, trace), F32),
            pltpu.VMEM((2 * here, trace), F32),
            pltpu.VMEM((2 * here, trace), BF16),
            pltpu.VMEM((2 * here, trace), BF16),
            pltpu.VMEM((2 * here, trace), F32),
            pltpu.VMEM((2 * cps, trace), F32),
            pltpu.VMEM((2, 4 * cps, 256), F32),
            pltpu.VMEM((4 * cps, trace), BF16),
            pltpu.VMEM((2, 3 * cps, trace), BF16),
            pltpu.VMEM((2 * cps, trace), F32),
            pltpu.VMEM((2 * cps, 2 * pair), F32),
            pltpu.VMEM((2, 2, 9 * cps, pair), BF16),
            pltpu.VMEM((2, 3 * cps, pair), BF16),
            pltpu.VMEM((cps, 5 * cps), F32),
            pltpu.VMEM((cps, 128), BF16),
            pltpu.VMEM((4, cps, 128), BF16),
            pltpu.VMEM((3, nz, nm, nc, cps // 2, 128), BF16),
            pltpu.VMEM((2, nz, 1, 128), F32),
            pltpu.VMEM((2, nm * nc, 1, 128), F32),
            pltpu.SemaphoreType.DMA((5,)),
            pltpu.SemaphoreType.DMA((copies,)),
            pltpu.SemaphoreType.DMA((copies,)),
        ],
        compiler_params=pltpu.CompilerParams(
            collective_id=0, has_side_effects=True, vmem_limit_bytes=50 * 1024 * 1024
        ),
    )(
        lead_side.reshape(2),
        keep(sources.reshape(2 * here, trace)),
        keep(impedance.reshape(2 * trace, trace)),
        keep(pair_maps.reshape(4, pair, pair)),
        keep(coarse_basis[0, 0]),
        keep(coarse_inverse),
    )
    return out.reshape(1, 1, 2, here, trace)


SHAPE = (8, 2, 4, 2, 2)


def build(mesh, shape):
    return jax.shard_map(
        functools.partial(per_device, shape),
        mesh=mesh,
        in_specs=(
            P("gx", "gy", None, "col", None),
            P("gx", "gy", None, None, None),
            P("gx", "gy", None, None, None, None),
            P("gx", "gy", None),
            P("gx", "gy", None, None, None),
            P(("gx", "gy", "col"), None),
        ),
        out_specs=P("gx", "gy", None, "col", None),
        check_vma=False,
    )


def solution(mesh):
    return build(mesh, SHAPE)
```

```python
import functools

import jax
import jax.numpy as jnp
from jax import lax
from jax.experimental import pallas as pl
from jax.experimental.pallas import tpu as pltpu
from jax.sharding import PartitionSpec as P

STEP_RATIO = 0.4
MESH = pl.DeviceIdType.MESH
F32 = jnp.float32
BF16 = jnp.bfloat16
HIGHEST = lax.Precision.HIGHEST


def dot(a, b, precision=None):
    return jnp.dot(a, b, preferred_element_type=F32, precision=precision)


def dot_nt(a, b, precision=None):
    return lax.dot_general(
        a, b, (((1,), (1,)), ((), ())), preferred_element_type=F32, precision=precision
    )


def dot_tn(a, b):
    return lax.dot_general(a, b, (((0,), (0,)), ((), ())), preferred_element_type=F32)


def split(x):
    high = x.astype(BF16)
    return high, (x - high.astype(F32)).astype(BF16)


def dot_three(a, b):
    high, low = split(a)
    b_high, b_low = split(b)
    first = dot(jnp.concatenate([high, low], axis=0), b_high)
    return first[: a.shape[0]] + first[a.shape[0] :] + dot(high, b_low)


def kernel(
    shape,
    lead_ref,
    src_hbm,
    imp_hbm,
    maps_hbm,
    basis_hbm,
    inv_hbm,
    out_ref,
    src,
    imp,
    maps,
    basis,
    inv,
    solver,
    inv_all,
    outgoing,
    image_out,
    face_out,
    face_in,
    image_in,
    ret_out,
    ret_in,
    solved_own,
    updated,
    state,
    rows,
    rows_turned,
    product,
    image,
    image_solved,
    proj_rows,
    basis_k,
    mapped,
    mapped_near,
    mapped_k,
    mapped_end,
    kernel_t,
    near_out,
    near_in,
    gathered,
    sum_z,
    sum_q,
    load_sem,
    send_sem,
    recv_sem,
):
    nz, nh, ny, nc, ncol = shape
    nm = nh * ny
    ngx, ngy = nz * nh, ny * nc
    sources = src.shape[0] // 2
    trace = src.shape[1]
    face = trace // 6
    pair = 2 * face
    cps = basis.shape[0]
    half = cps // 2

    gx, gy, col = lax.axis_index("gx"), lax.axis_index("gy"), lax.axis_index("col")
    z, xh = gx // nh, gx % nh
    y, core = gy // nc, gy % nc
    m = xh * ny + y

    def at(z_to, m_to, core_to):
        return {
            "gx": z_to * nh + m_to // ny,
            "gy": (m_to % ny) * nc + core_to,
            "col": col,
        }

    z_peers = [at((z + o) % nz, m, core) for o in range(1, nz)]
    m_peers = [at(z, (m + o) % nm, core) for o in range(1, nm)]
    c_peers = [at(z, m, (core + o) % nc) for o in range(1, nc)]
    q, nq = m * nc + core, nm * nc
    q_peers = [at(z, (q + o) % nq // nc, (q + o) % nq % nc) for o in range(1, nq)]
    offsets = [0]
    for o in range(1, nz // 2 + 1):
        offsets += [o] if 2 * o == nz else [o, nz - o]
    bounds = [0, 1] + list(range(3, nz - 2, 2)) + ([nz] if nz > 1 else [])
    groups = list(zip(bounds, bounds[1:]))
    below = [
        {"gx": (gx + ngx - 1) % ngx, "gy": gy, "col": col},
        {"gx": gx, "gy": (gy + ngy - 1) % ngy, "col": col},
    ]
    above = [
        {"gx": (gx + 1) % ngx, "gy": gy, "col": col},
        {"gx": gx, "gy": (gy + 1) % ngy, "col": col},
    ]
    col_peer = {"gx": gx, "gy": gy, "col": (col + 1) % ncol}
    position, last = [gx, gy], [ngx - 1, ngy - 1]

    loads = [
        pltpu.make_async_copy(a, b, load_sem.at[i])
        for i, (a, b) in enumerate(
            [(src_hbm, src), (maps_hbm, maps), (basis_hbm, basis), (inv_hbm, inv), (imp_hbm, imp)]
        )
    ]
    loads[0].start()

    barrier = pltpu.get_barrier_semaphore()
    partners = below + above + z_peers + q_peers + [col_peer]
    for partner in partners:
        pl.semaphore_signal(barrier, inc=1, device_id=partner, device_id_type=MESH)
    for i in (3, 1, 2, 4):
        loads[i].start()

    sent = []

    def remote(source, target, device):
        k = len(sent)
        copy = pltpu.make_async_remote_copy(
            src_ref=source,
            dst_ref=target,
            send_sem=send_sem.at[k],
            recv_sem=recv_sem.at[k],
            device_id=device,
            device_id_type=MESH,
        )
        copy.start()
        sent.append(copy)
        return copy

    def arrive(copies):
        for copy in copies:
            copy.wait_recv()

    def lanes(n):
        return lax.broadcasted_iota(jnp.int32, (n, 128), 1)

    def turned(x):
        part = x.shape[0] // 2
        return jnp.concatenate([-x[part:], x[:part]], axis=0)

    def packed_face(x):
        part = x.shape[0] // 2
        tail = jnp.where(
            lanes(part) < 64, x[:part, 128:256], pltpu.roll(x[part:, 128:256], 64, 1)
        )
        return jnp.concatenate([x[:, :128], tail], axis=0).astype(BF16)

    def face_parts(x):
        size = 2 * x.shape[0] // 3
        tail = x[size:].astype(F32)
        return x[:size].astype(F32), jnp.concatenate([tail, pltpu.roll(tail, 64, 1)], axis=0)

    def send_face(it, d):
        face_out[it, d] = packed_face(outgoing[it, :, pl.ds(d * pair, 256)].astype(F32))
        return remote(face_out.at[it, d], face_in.at[it, d], below[d])

    def solve(it, d, coming):
        coming[d].wait_recv()
        head, tail = face_parts(face_in[it, d])
        here = outgoing[it, :, pl.ds(d * pair, pair)]
        middle = jnp.where(lanes(2 * sources) < 64, tail, here[:, 128:256].astype(F32))
        x = jnp.concatenate([head.astype(BF16), middle.astype(BF16), here[:, 256:]], axis=1)
        solved = dot(x, solver[d, 0]) + dot(turned(x), solver[d, 1])
        ret_out[it, d] = packed_face(solved)
        solved_own[d] = solved[:, 128:]
        return remote(ret_out.at[it, d], ret_in.at[it, d], above[d])

    def assemble(it, returned):
        ends = outgoing[it, :, pl.ds(2 * pair, pair)].astype(F32)
        updated[it, :, pl.ds(2 * pair, pair)] = pltpu.roll(ends, face, 1)
        for d in range(2):
            returned[d].wait_recv()
            head, tail = face_parts(ret_in[it, d])
            own = jnp.where(position[d] < last[d], solved_own[d], 0.0)
            updated[it, :, pl.ds(d * pair, 128)] = jnp.where(position[d] > 0, head, 0.0)
            updated[it, :, pl.ds(d * pair + 128, 128)] = jnp.where(
                lanes(2 * sources) < 64, jnp.where(position[d] > 0, tail, 0.0), own[:, :128]
            )
            updated[it, :, pl.ds(d * pair + 256, 128)] = own[:, 128:]

    def apply_map(j):
        span = pl.ds(384 * j, 384)
        return dot(rows[...], imp[pl.ds(0, trace), span]) + dot(
            rows_turned[...], imp[pl.ds(trace, trace), span]
        )

    def packed(total):
        return jnp.where(
            lanes(half) < 64, total[:half], pltpu.roll(total[half:], sources, 1)
        ).astype(BF16)

    def project(defect):
        high, low = split(defect)
        first = dot_nt(proj_rows[...], high)
        second = dot_nt(proj_rows[pl.ds(0, 2 * cps), :], low)
        by_part = first[: 2 * cps] + first[2 * cps :] + second
        return packed(by_part[:cps] + pltpu.roll(by_part[cps:], sources, 1))

    def source_sums(products):
        folded = products[:, :128]
        for t in range(1, trace // 128):
            folded = folded + products[:, 128 * t : 128 * (t + 1)]
        folded = folded[:sources] + folded[sources:]
        both = jnp.concatenate([folded, folded], axis=0)
        return dot_nt(jnp.ones((8, 128), F32), both, HIGHEST)

    def forward(it, low, high):
        block = gathered.at[it, pl.ds(low, high - low), m, core]
        return [remote(block, block, peer) for peer in m_peers]

    def gather_start(it, block):
        gathered[it, 0, m, core] = block
        own = gathered.at[it, 0, m, core]
        coming = [None] * nz
        for i in range(nz - 1, 0, -1):
            coming[i] = remote(own, gathered.at[it, i, m, core], z_peers[offsets[i] - 1])
        return coming

    def gather_group(it, coming, low, high):
        arrive(coming[max(low, 1) : high])
        return forward(it, low, high)

    def gather_core(it, coming, low, high):
        arrive(coming)
        block = gathered.at[it, pl.ds(low, high - low), :, core]
        return [remote(block, block, peer) for peer in c_peers]

    def coarse_of(it, coming):
        arrive(coming)
        parts = 0.0
        for i in range(nz):
            parts = parts + dot(
                inv_all[i].reshape(2 * cps, nq * half), gathered[it, i].reshape(nq * half, 128)
            )
        return parts[:cps] + pltpu.roll(parts[cps:], sources, 1)

    def share(buffer, it, index, peers, row):
        buffer[it, index] = row[0:1]
        own = buffer.at[it, index]
        return [remote(own, own, peer) for peer in peers]

    def added(buffer, it, coming):
        arrive(coming)
        row = buffer[it, 0]
        for i in range(1, buffer.shape[1]):
            row = row + buffer[it, i]
        return jnp.broadcast_to(row, (8, 128))

    def stacked(coefficients):
        high, low = split(coefficients)
        return jnp.concatenate([high, low, high], axis=0)[:, :sources]

    def factor_of(total):
        return STEP_RATIO * jnp.sqrt(total / (pltpu.roll(total, sources, 1) + 1e-06))

    def energy_of(coarse):
        energy = jnp.sum(coarse * dot_three(gram, coarse), axis=0, keepdims=True)
        return pltpu.roll(jnp.broadcast_to(energy, (8, 128)), sources, 1)

    def three(block):
        high, low = split(block)
        return jnp.concatenate([high, high, low], axis=0)

    def mapped_sum(near, c, d):
        if d == 2:
            return dot_tn(stacked(near[0]), mapped_end[c])
        coefficients = jnp.concatenate(
            [stacked(near[0]), stacked(near[1 + 2 * d]), stacked(near[2 + 2 * d])], axis=0
        )
        return dot_tn(coefficients, mapped_k[c, d])

    def against_basis(block, c, start, width):
        high, low = split(block)
        first = dot_nt(
            jnp.concatenate([high, low], axis=0),
            proj_rows[pl.ds(c * cps, cps), pl.ds(start, width)],
        )
        second = dot_nt(high, proj_rows[pl.ds((2 + c) * cps, cps), pl.ds(start, width)])
        return first[: block.shape[0]] + first[block.shape[0] :] + second

    def sides_of(c, d):
        part = mapped_near[pl.ds(c * cps, cps), pl.ds(d * pair, pair)]
        left = lax.broadcasted_iota(jnp.int32, (cps, pair), 1) < face
        return jnp.concatenate([jnp.where(left, part, 0.0), jnp.where(left, 0.0, part)], axis=0)

    loads[0].wait()
    outgoing[0] = src[...].astype(BF16)
    pl.semaphore_wait(barrier, len(partners))
    faces = [send_face(0, d) for d in range(2)]

    loads[2].wait()
    both = jnp.concatenate([basis[:, 0, :], basis[:, 1, :]], axis=0)
    high, low = split(both)
    proj_rows[pl.ds(0, 2 * cps), :] = high
    proj_rows[pl.ds(2 * cps, 2 * cps), :] = low
    for part, block in enumerate((high, low)):
        rows[pl.ds(part * 2 * cps, 2 * cps), :] = block
        rows_turned[pl.ds(part * 2 * cps, 2 * cps), :] = turned(block)

    loads[4].wait()

    def apply_to_basis(j):
        whole = apply_map(j)
        whole = whole[: 2 * cps] + whole[2 * cps :]
        image[:, pl.ds(384 * j, 384)] = whole
        return whole

    image_coming = []

    def send_image(j):
        image_out[j] = packed_face(apply_to_basis(j))
        image_coming.append(remote(image_out.at[j], image_in.at[j], below[j]))

    send_image(0)
    loads[1].wait()
    for d in range(2):
        for c in range(2):
            stored = maps[2 * d + c].astype(F32)
            swapped = jnp.concatenate([stored[face:], stored[:face]], axis=0)
            swapped = pltpu.roll(swapped, face, 1)
            solver[d, c] = jnp.where(lead_ref[d] == 0, swapped, stored).astype(BF16)
    returned = [solve(0, 0, faces)]
    send_image(1)
    returned.append(solve(0, 1, faces))
    apply_to_basis(2)

    loads[3].wait()
    here = lax.broadcasted_iota(jnp.int32, (256, 256), 0)
    there = lax.broadcasted_iota(jnp.int32, (256, 256), 1)
    wanted = ((here // half) % 2) * 128 + (here // cps) * half + here % half
    order = jnp.where(there == wanted, 1.0, 0.0).astype(BF16)
    chunks = nq * cps // 256
    for i in range(nz):
        source_z = (z + nz - offsets[i]) % nz
        for j in range(chunks):
            start = pl.multiple_of((source_z * chunks + j) * 256, 256)
            moved = dot(inv[:, pl.ds(start, 256)].astype(BF16), order).astype(BF16)
            for h in range(2):
                inv_all[i, h, col, :, pl.ds(128 * j, 128)] = moved[:, 128 * h : 128 * (h + 1)]

    image_returned = []
    for d in range(2):
        image_coming[d].wait_recv()
        head, tail = face_parts(image_in[d])
        own = image[:, pl.ds(d * pair, pair)]
        low_lane = lanes(2 * cps) < 64
        zero = jnp.zeros((2 * cps, 128), F32)
        x = jnp.concatenate(
            [zero, jnp.where(low_lane, 0.0, own[:, 128:256]), own[:, 256:]], axis=1
        ).astype(BF16)
        w = jnp.concatenate(
            [head, jnp.where(low_lane, tail, 0.0), zero], axis=1
        ).astype(BF16)
        solved = dot(jnp.concatenate([x, w], axis=0), solver[d, 0]) + dot(
            jnp.concatenate([turned(x), turned(w)], axis=0), solver[d, 1]
        )
        ret_out[2, d] = packed_face(solved)
        image_solved[d] = solved[:, 128:]
        image_returned.append(remote(ret_out.at[2, d], ret_in.at[2, d], above[d]))
    assemble(0, returned)

    coming = gather_start(0, project(updated[0]))
    inverse_coming = remote(inv_all.at[:, :, col], inv_all.at[:, :, col], col_peer)
    moving = [gather_group(0, coming, *groups[0])]
    high = updated[0].astype(BF16)
    rows[...] = high
    rows_turned[...] = turned(high)
    faces_next = []
    for j in range(trace // 384):
        if j == 2:
            for group in groups[3:]:
                moving.append(gather_group(0, coming, *group))
        span = pl.ds(384 * j, 384)
        outgoing[1, :, span] = (apply_map(j) + src[:, span]).astype(BF16)
        if j < 2:
            faces_next.append(send_face(1, j))
            if j + 1 < len(groups):
                moving.append(gather_group(0, coming, *groups[j + 1]))

    first_squares = source_sums(updated[0] * updated[0])
    gram = dot_nt(both[:cps], both[:cps], HIGHEST) + dot_nt(both[cps:], both[cps:], HIGHEST)
    for c in range(2):
        basis_k[c] = three(both[c * cps : (c + 1) * cps])
    split_at = groups[-1][0]
    returned = [solve(1, d, faces_next) for d in range(2)]
    coming = gather_core(0, sum(moving[:-1], []), 0, split_at)
    coming += gather_core(0, moving[-1], split_at, nz)

    inverse_coming.wait_recv()
    coarse = coarse_of(0, coming)
    high, low = split(coarse)
    near_out[...] = jnp.where(
        lanes(cps) < 64, high.astype(F32), pltpu.roll(low.astype(F32), sources, 1)
    ).astype(BF16)
    near_coming = []
    for d in range(2):
        near_coming.append(remote(near_out, near_in.at[2 * d], above[d]))
        near_coming.append(remote(near_out, near_in.at[2 * d + 1], below[d]))
    first_row = jnp.where(lanes(8) < 64, first_squares, energy_of(coarse))
    for d in range(2):
        image_returned[d].wait_recv()
        back = jnp.concatenate(face_parts(ret_in[2, d]), axis=1)
        back = jnp.where(position[d] > 0, back, 0.0)
        own = jnp.where(position[d] < last[d], image_solved[d], 0.0)
        for target, r, o in ((mapped, 2 * cps, 0), (mapped_near, 0, 2 * cps)):
            target[:, pl.ds(d * pair, 128)] = back[r : r + 2 * cps, :128]
            target[:, pl.ds(d * pair + 128, 128)] = jnp.where(
                lanes(2 * cps) < 64, back[r : r + 2 * cps, 128:], own[o : o + 2 * cps, :128]
            )
            target[:, pl.ds(d * pair + 256, 128)] = own[o : o + 2 * cps, 128:]
    mapped[:, pl.ds(2 * pair, pair)] = pltpu.roll(image[:, pl.ds(2 * pair, pair)], face, 1)
    moved = mapped[...] - both
    blocks = [
        against_basis(moved[:cps], 0, 0, trace) + against_basis(moved[cps:], 1, 0, trace)
    ]
    for d in range(2):
        blocks.append(
            against_basis(sides_of(0, d), 0, d * pair, pair)
            + against_basis(sides_of(1, d), 1, d * pair, pair)
        )
    kernel_t[...] = jnp.concatenate(blocks, axis=0).T


    assemble(1, returned)
    state[...] = updated[1] - updated[0]
    early = gather_start(2, project(state[...]))

    arrive(near_coming)
    near = [coarse]
    for i in range(4):
        both_parts = near_in[i].astype(F32)
        near.append(both_parts + pltpu.roll(both_parts, sources, 1))
    coming = gather_start(
        1, packed(dot_three(kernel_t[...], jnp.concatenate(near, axis=0)))
    )
    norms = share(sum_z, 0, z, z_peers, first_row)
    moving = [gather_group(1, coming, *groups[0])]
    for c in range(2):
        for d in range(2):
            sides = sides_of(c, d)
            own = three(mapped[pl.ds(c * cps, cps), pl.ds(d * pair, pair)])
            mapped_k[c, d] = jnp.concatenate(
                [own, three(sides[:cps]), three(sides[cps:])], axis=0
            )
        mapped_end[c] = three(mapped[pl.ds(c * cps, cps), pl.ds(2 * pair, pair)])
    early = gather_group(2, early, 0, nz)
    for c in range(2):
        part = pl.ds(c * sources, sources)
        for d in range(3):
            product[part, pl.ds(d * pair, pair)] = mapped_sum(near, c, d)
        product[part, :] = product[part, :] - dot_tn(stacked(coarse), basis_k[c])
        if c + 1 < len(groups):
            moving.append(gather_group(1, coming, *groups[c + 1]))
    for group in groups[3:]:
        moving.append(gather_group(1, coming, *group))
    norms = share(sum_q, 0, q, q_peers, added(sum_z, 0, norms))
    sums_aa = source_sums(state[...] * state[...])
    sums_ab = source_sums(state[...] * product[...])
    sums_bb = source_sums(product[...] * product[...])
    early = gather_core(2, early, 0, nz)
    late = gather_core(1, sum(moving[:-1], []), 0, split_at)
    coarse_early = coarse_of(2, early)
    late += gather_core(1, moving[-1], split_at, nz)
    factor = factor_of(added(sum_q, 0, norms))
    coarse = coarse_early + factor[0:1] * coarse_of(1, late)
    squares = sums_aa + factor * (2.0 * sums_ab + factor * sums_bb)
    row = jnp.where(lanes(8) < 64, squares, energy_of(coarse))
    norms = share(sum_z, 1, z, z_peers, row)
    near = [factor[0:1] * part for part in near]

    def finish_update(c):
        part = pl.ds(c * sources, sources)
        for d in range(3):
            span = pl.ds(d * pair, pair)
            updated[1, part, span] = updated[1, part, span] + mapped_sum(near, c, d)

    finish_update(0)
    norms = share(sum_q, 1, q, q_peers, added(sum_z, 1, norms))
    finish_update(1)
    factor = factor_of(added(sum_q, 1, norms))
    scaled = stacked(factor[0:1] * coarse)
    for c in range(2):
        part = pl.ds(c * sources, sources)
        out_ref[part, :] = updated[1, part, :] + dot_tn(scaled, basis_k[c])
    for copy in sent:
        copy.wait_send()


def per_device(shape, sources, impedance, pair_maps, lead_side, coarse_basis, coarse_inverse):
    nz, nh, ny, nc, ncol = shape
    here, trace = sources.shape[3], sources.shape[4]
    pair = pair_maps.shape[-1]
    cps = coarse_basis.shape[2]
    size = coarse_inverse.shape[1]
    nm = nh * ny
    copies = 1 + 3 * 4 + 4 + 3 * (nz - 1) + 9 * (nm - 1) + 5 * (nc - 1)
    copies += 2 * (nz - 1 + nm * nc - 1)
    def keep(array):
        return pltpu.with_memory_space_constraint(array, pltpu.HBM)

    hbm = pl.BlockSpec(memory_space=pltpu.HBM)
    out = pl.pallas_call(
        functools.partial(kernel, shape),
        out_shape=jax.ShapeDtypeStruct((2 * here, trace), F32),
        in_specs=[pl.BlockSpec(memory_space=pltpu.SMEM)] + [hbm] * 5,
        out_specs=pl.BlockSpec(memory_space=pltpu.VMEM),
        scratch_shapes=[
            pltpu.VMEM((2 * here, trace), F32),
            pltpu.VMEM((2 * trace, trace), BF16),
            pltpu.VMEM((4, pair, pair), BF16),
            pltpu.VMEM((cps, 2, trace), F32),
            pltpu.VMEM((cps // 2, size), F32),
            pltpu.VMEM((2, 2, pair, pair), BF16),
            pltpu.VMEM((nz, 2, ncol, cps // 2, nm * nc * cps // 2), BF16),
            pltpu.VMEM((2, 2 * here, trace), BF16),
            pltpu.VMEM((2, 3 * cps, 128), BF16),
            pltpu.VMEM((2, 2, 3 * here, 128), BF16),
            pltpu.VMEM((2, 2, 3 * here, 128), BF16),
            pltpu.VMEM((2, 3 * cps, 128), BF16),
            pltpu.VMEM((3, 2, 3 * here, 128), BF16),
            pltpu.VMEM((3, 2, 3 * here, 128), BF16),
            pltpu.VMEM((2, 2 * here, 256), F32),
            pltpu.VMEM((2, 2 * here, trace), F32),
            pltpu.VMEM((2 * here, trace), F32),
            pltpu.VMEM((2 * here, trace), BF16),
            pltpu.VMEM((2 * here, trace), BF16),
            pltpu.VMEM((2 * here, trace), F32),
            pltpu.VMEM((2 * cps, trace), F32),
            pltpu.VMEM((2, 4 * cps, 256), F32),
            pltpu.VMEM((4 * cps, trace), BF16),
            pltpu.VMEM((2, 3 * cps, trace), BF16),
            pltpu.VMEM((2 * cps, trace), F32),
            pltpu.VMEM((2 * cps, 2 * pair), F32),
            pltpu.VMEM((2, 2, 9 * cps, pair), BF16),
            pltpu.VMEM((2, 3 * cps, pair), BF16),
            pltpu.VMEM((cps, 5 * cps), F32),
            pltpu.VMEM((cps, 128), BF16),
            pltpu.VMEM((4, cps, 128), BF16),
            pltpu.VMEM((3, nz, nm, nc, cps // 2, 128), BF16),
            pltpu.VMEM((2, nz, 1, 128), F32),
            pltpu.VMEM((2, nm * nc, 1, 128), F32),
            pltpu.SemaphoreType.DMA((5,)),
            pltpu.SemaphoreType.DMA((copies,)),
            pltpu.SemaphoreType.DMA((copies,)),
        ],
        compiler_params=pltpu.CompilerParams(
            collective_id=0, has_side_effects=True, vmem_limit_bytes=50 * 1024 * 1024
        ),
    )(
        lead_side.reshape(2),
        keep(sources.reshape(2 * here, trace)),
        keep(impedance.reshape(2 * trace, trace)),
        keep(pair_maps.reshape(4, pair, pair)),
        keep(coarse_basis[0, 0]),
        keep(coarse_inverse),
    )
    return out.reshape(1, 1, 2, here, trace)


SHAPE = (8, 2, 4, 2, 2)


def build(mesh, shape):
    return jax.shard_map(
        functools.partial(per_device, shape),
        mesh=mesh,
        in_specs=(
            P("gx", "gy", None, "col", None),
            P("gx", "gy", None, None, None),
            P("gx", "gy", None, None, None, None),
            P("gx", "gy", None),
            P("gx", "gy", None, None, None),
            P(("gx", "gy", "col"), None),
        ),
        out_specs=P("gx", "gy", None, "col", None),
        check_vma=False,
    )


def solution(mesh):
    return build(mesh, SHAPE)
```
